32 devices in a mesh: dp: 2 (over x), sp: 4 (over z), uly: 4 (over y, core).
Axes of the slice: x: 2, y: 2, z: 4, core: 2. Of those that a mesh axis runs over, the one named last changes fastest.
Arguments:
- tokens: bfloat16 [2, 4096, 1536], P('dp', ('sp', 'uly')), parts along dimension 0
- rope_ang: float32 [4096, 64], P(('sp', 'uly'))
- t_emb: float32 [2, 6, 1536], P('dp'), parts along dimension 0
- block_mod: float32 [1, 6, 1536], replicated
- context: bfloat16 [2, 512, 1536], P('dp'), parts along dimension 0
- attn_wq: bfloat16 [1536, 1536], replicated
- attn_bq: bfloat16 [1536], replicated
- attn_wk: bfloat16 [1536, 1536], replicated
- attn_bk: bfloat16 [1536], replicated
- attn_wv: bfloat16 [1536, 1536], replicated
- attn_bv: bfloat16 [1536], replicated
- attn_gq: bfloat16 [1536], replicated
- attn_gk: bfloat16 [1536], replicated
- attn_wo: bfloat16 [1536, 1536], replicated
- attn_bo: bfloat16 [1536], replicated
- norm3_w: bfloat16 [1536], replicated
- norm3_b: bfloat16 [1536], replicated
- cross_wq: bfloat16 [1536, 1536], replicated
- cross_wk: bfloat16 [1536, 1536], replicated
- cross_wv: bfloat16 [1536, 1536], replicated
- cross_gq: bfloat16 [1536], replicated
- cross_gk: bfloat16 [1536], replicated
- cross_wo: bfloat16 [1536, 1536], replicated
- ffn_w1: bfloat16 [1536, 8960], replicated
- ffn_w2: bfloat16 [8960, 1536], replicated
Outputs:
- output: bfloat16 [2, 4096, 1536], P('dp', ('sp', 'uly')), parts along dimension 0
There are 2 independent parts. The reference program is written for one: setup_inputs(seed, part) draws one part's arguments, and reference() takes and returns one part's arrays. A program takes and returns all parts, laid end to end along the dimension named above; an argument that names none is the same for every part.
All inputs are finite; a program needn't handle non-finite values.
Results may differ from the reference program's by a relative error of at most 0.00550236.
Values are sent between devices in bfloat16 or wider.
A program may use at most 1 GiB of HBM per device.

```python
import jax
import jax.numpy as jnp
from jax import lax

BATCH = 1
FRAMES = 4
ROWS = 16
COLS = 64
D = 1536
HEADS = 12
HEAD = 128
FF = 8960
TEXT = 512
SEQ = FRAMES * ROWS * COLS
FRAME_TOK = ROWS * COLS
EPS = 1e-6


def rope_table(table_key):
    frame_gaps = jax.random.randint(table_key, (FRAMES,), 1, 7)
    t_pos = (jnp.cumsum(frame_gaps) - frame_gaps[0]).astype(jnp.float32)
    h_pos = jnp.arange(ROWS).astype(jnp.float32)
    w_pos = jnp.arange(COLS).astype(jnp.float32)
    freq_t = 1.0 / (10000.0 ** (jnp.arange(0, 44, 2).astype(jnp.float32) / 44.0))
    freq_s = 1.0 / (10000.0 ** (jnp.arange(0, 42, 2).astype(jnp.float32) / 42.0))
    ang_t = jnp.broadcast_to((t_pos[:, None] * freq_t)[:, None, None, :], (FRAMES, ROWS, COLS, 22))
    ang_h = jnp.broadcast_to((h_pos[:, None] * freq_s)[None, :, None, :], (FRAMES, ROWS, COLS, 21))
    ang_w = jnp.broadcast_to((w_pos[:, None] * freq_s)[None, None, :, :], (FRAMES, ROWS, COLS, 21))
    return jnp.concatenate([ang_t, ang_h, ang_w], axis=-1).reshape(SEQ, 64)


def setup_inputs(seed: int = 0, part: int = 0) -> dict:
    root_key = jax.random.key(seed)
    part_keys = jax.random.split(jax.random.fold_in(root_key, part), 3)
    shared = jax.random.split(root_key, 24)

    def normal(sub_key, shape, scale):
        return jax.random.normal(sub_key, shape, jnp.float32) * scale

    scale_d = D ** -0.5
    scale_ff = FF ** -0.5
    return {
        'tokens': normal(part_keys[0], (BATCH, SEQ, D), 1.0).astype(jnp.bfloat16),
        'rope_ang': rope_table(shared[0]),
        't_emb': normal(part_keys[1], (BATCH, 6, D), 0.3),
        'block_mod': normal(shared[1], (1, 6, D), 0.3),
        'context': normal(part_keys[2], (BATCH, TEXT, D), 1.0).astype(jnp.bfloat16),
        'attn_wq': normal(shared[2], (D, D), scale_d).astype(jnp.bfloat16),
        'attn_bq': normal(shared[3], (D,), 0.5).astype(jnp.bfloat16),
        'attn_wk': normal(shared[4], (D, D), scale_d).astype(jnp.bfloat16),
        'attn_bk': normal(shared[5], (D,), 0.5).astype(jnp.bfloat16),
        'attn_wv': normal(shared[6], (D, D), scale_d).astype(jnp.bfloat16),
        'attn_bv': normal(shared[7], (D,), 0.5).astype(jnp.bfloat16),
        'attn_gq': (1.7 + normal(shared[8], (D,), 0.4)).astype(jnp.bfloat16),
        'attn_gk': (1.7 + normal(shared[9], (D,), 0.4)).astype(jnp.bfloat16),
        'attn_wo': normal(shared[10], (D, D), scale_d).astype(jnp.bfloat16),
        'attn_bo': normal(shared[11], (D,), 0.5).astype(jnp.bfloat16),
        'norm3_w': (1.0 + normal(shared[12], (D,), 0.3)).astype(jnp.bfloat16),
        'norm3_b': normal(shared[13], (D,), 0.5).astype(jnp.bfloat16),
        'cross_wq': normal(shared[14], (D, D), scale_d).astype(jnp.bfloat16),
        'cross_wk': normal(shared[15], (D, D), scale_d).astype(jnp.bfloat16),
        'cross_wv': normal(shared[16], (D, D), scale_d).astype(jnp.bfloat16),
        'cross_gq': (1.4 + normal(shared[17], (D,), 0.3)).astype(jnp.bfloat16),
        'cross_gk': (1.4 + normal(shared[18], (D,), 0.3)).astype(jnp.bfloat16),
        'cross_wo': normal(shared[19], (D, D), scale_d).astype(jnp.bfloat16),
        'ffn_w1': normal(shared[20], (D, FF), scale_d).astype(jnp.bfloat16),
        'ffn_w2': normal(shared[21], (FF, D), scale_ff).astype(jnp.bfloat16),
    }


def layer_norm(x_f32):
    mean_x = jnp.mean(x_f32, axis=-1, keepdims=True)
    centered = x_f32 - mean_x
    var_x = jnp.mean(centered * centered, axis=-1, keepdims=True)
    return centered * lax.rsqrt(var_x + EPS)


def rms_norm(h_lin, gain):
    return h_lin * lax.rsqrt(jnp.mean(h_lin * h_lin, axis=-1, keepdims=True) + EPS) * gain.astype(jnp.float32)


def apply_rope(heads, cos_ang, sin_ang):
    pairs = heads.reshape(heads.shape[:-1] + (HEAD // 2, 2))
    pair_a = pairs[..., 0]
    pair_b = pairs[..., 1]
    turned = jnp.stack([pair_a * cos_ang - pair_b * sin_ang, pair_a * sin_ang + pair_b * cos_ang], axis=-1)
    return turned.reshape(heads.shape)


def project(operand, weight):
    flat = jnp.dot(operand.reshape(-1, operand.shape[-1]), weight, preferred_element_type=jnp.float32)
    return flat.reshape(operand.shape[:-1] + (weight.shape[-1],))


def attend_block(q_blk, k_f32, v_f32):
    scores = jnp.einsum('bqd,bkd->bqk', q_blk.astype(jnp.float32), k_f32) * (HEAD ** -0.5)
    weights = jnp.exp(scores - jnp.max(scores, axis=-1, keepdims=True))
    weighted_v = jnp.einsum('bqk,bkd->bqd', weights.astype(jnp.bfloat16).astype(jnp.float32), v_f32)
    return (weighted_v / jnp.sum(weights, axis=-1, keepdims=True)).astype(jnp.bfloat16)


def reference(tokens, rope_ang, t_emb, block_mod, context, attn_wq, attn_bq, attn_wk, attn_bk, attn_wv, attn_bv, attn_gq, attn_gk, attn_wo, attn_bo, norm3_w, norm3_b, cross_wq, cross_wk, cross_wv, cross_gq, cross_gk, cross_wo, ffn_w1, ffn_w2):
    ada_mod = t_emb + block_mod
    shift1 = ada_mod[:, 0:1]
    scale1 = ada_mod[:, 1:2]
    gate1 = ada_mod[:, 2:3]
    shift2 = ada_mod[:, 3:4]
    scale2 = ada_mod[:, 4:5]
    gate2 = ada_mod[:, 5:6]
    x_res = tokens.astype(jnp.float32)
    y_mod = (layer_norm(x_res) * (1.0 + scale1) + shift1).astype(jnp.bfloat16)
    cos_ang = jnp.cos(rope_ang)[:, None, :]
    sin_ang = jnp.sin(rope_ang)[:, None, :]
    head_shape = (BATCH, SEQ, HEADS, HEAD)
    q_tok = apply_rope(rms_norm(project(y_mod, attn_wq) + attn_bq.astype(jnp.float32), attn_gq).reshape(head_shape), cos_ang, sin_ang).astype(jnp.bfloat16)
    k_tok = apply_rope(rms_norm(project(y_mod, attn_wk) + attn_bk.astype(jnp.float32), attn_gk).reshape(head_shape), cos_ang, sin_ang).astype(jnp.bfloat16)
    v_tok = (project(y_mod, attn_wv) + attn_bv.astype(jnp.float32)).astype(jnp.bfloat16).reshape(head_shape)

    q_heads = jnp.moveaxis(q_tok, 2, 0).reshape(HEADS, BATCH, FRAMES, FRAME_TOK, HEAD)
    k_heads = jnp.moveaxis(k_tok, 2, 0)
    v_heads = jnp.moveaxis(v_tok, 2, 0)

    def self_head(operands):
        q_one, k_one, v_one = operands
        k_f32 = k_one.astype(jnp.float32)
        v_f32 = v_one.astype(jnp.float32)
        return lax.map(lambda q_frame: attend_block(q_frame, k_f32, v_f32), jnp.moveaxis(q_one, 1, 0))

    self_out = lax.map(self_head, (q_heads, k_heads, v_heads))
    attn_out = jnp.transpose(self_out, (2, 1, 3, 0, 4)).reshape(BATCH, SEQ, D)
    x_one = x_res + gate1 * (project(attn_out, attn_wo) + attn_bo.astype(jnp.float32))

    z_norm = (layer_norm(x_one) * norm3_w.astype(jnp.float32) + norm3_b.astype(jnp.float32)).astype(jnp.bfloat16)
    text_shape = (BATCH, TEXT, HEADS, HEAD)
    cross_q = rms_norm(project(z_norm, cross_wq), cross_gq).astype(jnp.bfloat16).reshape(head_shape)
    cross_k = rms_norm(project(context, cross_wk), cross_gk).astype(jnp.bfloat16).reshape(text_shape)
    cross_v = project(context, cross_wv).astype(jnp.bfloat16).reshape(text_shape)

    def cross_head(operands):
        q_one, k_one, v_one = operands
        return attend_block(q_one, k_one.astype(jnp.float32), v_one.astype(jnp.float32))

    cross_out = lax.map(cross_head, (jnp.moveaxis(cross_q, 2, 0), jnp.moveaxis(cross_k, 2, 0), jnp.moveaxis(cross_v, 2, 0)))
    cross_tok = jnp.transpose(cross_out, (1, 2, 0, 3)).reshape(BATCH, SEQ, D)
    x_two = x_one + project(cross_tok, cross_wo)

    def ffn_frame(x_frame):
        hidden = (layer_norm(x_frame) * (1.0 + scale2) + shift2).astype(jnp.bfloat16)
        gelu_out = jax.nn.gelu(project(hidden, ffn_w1), approximate=True).astype(jnp.bfloat16)
        return (x_frame + gate2 * project(gelu_out, ffn_w2)).astype(jnp.bfloat16)

    frames_out = lax.map(ffn_frame, jnp.moveaxis(x_two.reshape(BATCH, FRAMES, FRAME_TOK, D), 1, 0))
    return jnp.moveaxis(frames_out, 0, 1).reshape(BATCH, SEQ, D)
```

```python
import functools
import math

import jax
import jax.numpy as jnp
from jax import lax
from jax.experimental import pallas as pl
from jax.experimental.pallas import tpu as pltpu
from jax.sharding import PartitionSpec as P

EPS = 1e-6
HEAD = 128
D = 1536
TOK = 256
HALF = 768
DUAL = 48
AUX = 136
MESH = pl.DeviceIdType.MESH
EXP_SCALE = math.log2(math.e) * HEAD ** -0.5
F32 = jnp.float32
BF16 = jnp.bfloat16


def rope_parts(packed_ang):
    lane = lax.broadcasted_iota(jnp.int32, (128, 128), 1)
    pair = lane // 2
    sign = jnp.where(lane % 2 == 0, -1.0, 1.0).astype(F32)
    cos_p = jnp.cos(packed_ang)
    sin_p = jnp.sin(packed_ang)
    parts = []
    for base in (0, 64):
        parts.append((jnp.take_along_axis(cos_p, pair + base, axis=1),
                      jnp.take_along_axis(sin_p, pair + base, axis=1) * sign))
    return parts


def swap_pairs(val):
    lane = lax.broadcasted_iota(jnp.int32, val.shape, 1)
    return jnp.where(lane % 2 == 0, pltpu.roll(val, 127, 1), pltpu.roll(val, 1, 1))


def pre_kernel(x_ref, temb_ref, mod_ref, ang_ref, wq_ref, wk_ref, bq_ref, bk_ref, gq_ref,
               y_ref, q_ref, aux_ref, q_raw, ssq_q, ssq_k):
    step = pl.program_id(0)

    @pl.when(step == 0)
    def _():
        shift = temb_ref[0, 0:1] + mod_ref[0, 0:1]
        scale = 1.0 + (temb_ref[0, 1:2] + mod_ref[0, 1:2])

        @pl.loop(0, TOK // 32)
        def _(part):
            rows = pl.ds(part * 32, 32)
            x_f32 = x_ref[0, rows].astype(F32)
            centered = x_f32 - jnp.mean(x_f32, axis=-1, keepdims=True)
            var = jnp.mean(centered * centered, axis=-1, keepdims=True)
            y_ref[rows] = (centered * lax.rsqrt(var + EPS) * scale + shift).astype(BF16)
        ssq_q[...] = jnp.zeros_like(ssq_q)
        ssq_k[...] = jnp.zeros_like(ssq_k)

    q_lin = jnp.dot(y_ref[...], wq_ref[...], preferred_element_type=F32) + bq_ref[...].astype(F32)
    k_lin = jnp.dot(y_ref[...], wk_ref[...], preferred_element_type=F32) + bk_ref[...].astype(F32)
    q_raw[step] = q_lin
    ssq_q[...] += q_lin[:, :128] * q_lin[:, :128] + q_lin[:, 128:] * q_lin[:, 128:]
    ssq_k[...] += k_lin[:, :128] * k_lin[:, :128] + k_lin[:, 128:] * k_lin[:, 128:]

    @pl.when(step == pl.num_programs(0) - 1)
    def _():
        packed = ang_ref[...]
        aux_ref[0:128] = packed
        k_inv = lax.rsqrt(jnp.sum(ssq_k[...], axis=1, keepdims=True) * (1.0 / D) + EPS)
        for part in (0, 1):
            wide = jnp.broadcast_to(k_inv[part * 128:(part + 1) * 128], (128, 128))
            aux_ref[128 + part:129 + part] = wide.T[0:1]
        aux_ref[130:136] = jnp.zeros((6, 128), F32)
        q_inv = lax.rsqrt(jnp.sum(ssq_q[...], axis=1, keepdims=True) * (1.0 / D) + EPS)
        parts = rope_parts(packed)
        for head in range(D // HEAD):
            cols = pl.ds((head % 2) * 128, 128)
            out_cols = pl.ds((head % 6) * 128, 128)
            gain = gq_ref[:, head * 128:(head + 1) * 128].astype(F32)
            for part in (0, 1):
                rows = pl.ds(part * 128, 128)
                val = q_raw[head // 2, rows, cols] * q_inv[part * 128:(part + 1) * 128] * gain
                cos_d, sin_d = parts[part]
                q_ref[head // 6, rows, out_cols] = (val * cos_d + swap_pairs(val) * sin_d).astype(BF16)


def pre(x, t_emb, block_mod, packed_ang, wq, wk, bq, bk, gq):
    vec = lambda: pl.BlockSpec((1, 256), lambda j: (0, j))
    const = lambda shape: pl.BlockSpec(shape, lambda j: (0,) * len(shape))
    return pl.pallas_call(
        pre_kernel,
        grid=(6,),
        out_shape=[jax.ShapeDtypeStruct((TOK, D), BF16), jax.ShapeDtypeStruct((2, TOK, HALF), BF16),
                   jax.ShapeDtypeStruct((AUX, 128), F32)],
        in_specs=[const((1, TOK, D)), const((1, 6, D)), const((1, 6, D)), const((128, 128)),
                  pl.BlockSpec((D, 256), lambda j: (0, j)), pl.BlockSpec((D, 256), lambda j: (0, j)),
                  vec(), vec(), const((1, D))],
        out_specs=[const((TOK, D)), const((2, TOK, HALF)), const((AUX, 128))],
        scratch_shapes=[pltpu.VMEM((6, TOK, 256), F32), pltpu.VMEM((TOK, 128), F32), pltpu.VMEM((TOK, 128), F32)],
        cost_estimate=pl.CostEstimate(flops=4 * TOK * D * D, bytes_accessed=4 * D * D + 6 * TOK * D, transcendentals=0),
        compiler_params=pltpu.CompilerParams(vmem_limit_bytes=40 << 20),
        name="pre",
    )(x, t_emb, block_mod, packed_ang, wq, wk, bq, bk, gq)


def attn_kernel(y_hbm, aux_hbm, q_hbm, wk_hbm, wv_hbm, bk_ref, gk_ref, bv_ref, o_hbm,
                ybuf, abuf, qbuf, q_t, wk_v, wv_v, k_b, v_b, cos_b, sin_b, inv_b, acc, m_s, l_s, obuf,
                rs_main, rs_dual, rs_aux, ss, loc, qo_s, qo_r):
    z = lax.axis_index('sp')
    u = lax.axis_index('uly')
    yy = u // 2
    cc = u % 2
    hi = z // 2
    zm = z * (1 - hi) + (3 - z) * hi
    dev_up = {'sp': (z + 1) % 4, 'uly': u}
    dev_dn = {'sp': (z + 3) % 4, 'uly': u}
    dev_y = {'sp': z, 'uly': (1 - yy) * 2 + cc}
    dev_c = {'sp': z, 'uly': yy * 2 + 1 - cc}
    UP, DN, YP, CP = 0, 1, 2, 3
    dev = (dev_up, dev_dn, dev_y, dev_c)

    def z_of(i):
        low = i // 2
        m_i = low * i + (1 - low) * (i + zm - 2 * i * zm)
        return m_i * (1 - hi) + (3 - m_i) * hi

    def slot_a(i):
        return z_of(i) * 4 + yy * 2 + cc

    def slot_b(i):
        return z_of(i) * 4 + (1 - yy) * 2 + cc

    def slot_c(i):
        return z_of(i) * 4 + yy * 2 + 1 - cc

    def slot_d(i):
        return z_of(i) * 4 + (1 - yy) * 2 + 1 - cc

    def full(slot, to):
        ref = ybuf.at[slot]
        return pltpu.make_async_remote_copy(ref, ref, ss.at[to, 0, slot], rs_main.at[slot], device_id=dev[to], device_id_type=MESH)

    def main(slot, to):
        ref = ybuf.at[slot, pl.ds(DUAL, TOK - DUAL)]
        return pltpu.make_async_remote_copy(ref, ref, ss.at[to, 0, slot], rs_main.at[slot], device_id=dev[to], device_id_type=MESH)

    def dual(slot, to):
        ref = ybuf.at[slot, pl.ds(0, DUAL)]
        return pltpu.make_async_remote_copy(ref, ref, ss.at[to, 1, slot], rs_dual.at[slot], device_id=dev[to], device_id_type=MESH)

    def aux(slot, to):
        ref = abuf.at[slot]
        return pltpu.make_async_remote_copy(ref, ref, ss.at[to, 2, slot], rs_aux.at[slot], device_id=dev[to], device_id_type=MESH)

    barrier = pltpu.get_barrier_semaphore()
    pl.semaphore_signal(barrier, 1, device_id=dev_y, device_id_type=MESH)
    pl.semaphore_signal(barrier, 1, device_id=dev_c, device_id_type=MESH)

    @pl.when(z < 3)
    def _():
        pl.semaphore_signal(barrier, 1, device_id=dev_up, device_id_type=MESH)

    @pl.when(z > 0)
    def _():
        pl.semaphore_signal(barrier, 1, device_id=dev_dn, device_id_type=MESH)

    mine = slot_a(0)
    own_y = pltpu.make_async_copy(y_hbm, ybuf.at[mine], loc.at[0])
    own_a = pltpu.make_async_copy(aux_hbm, abuf.at[mine], loc.at[1])
    own_q = pltpu.make_async_copy(q_hbm.at[cc], qbuf.at[cc], loc.at[2])
    cols = pl.ds(pl.multiple_of(cc * HALF, 128), HALF)
    get_wk = pltpu.make_async_copy(wk_hbm.at[:, cols], wk_v, loc.at[3])
    get_wv = pltpu.make_async_copy(wv_hbm.at[:, cols], wv_v, loc.at[4])
    own_y.start()
    own_a.start()
    own_q.start()
    get_wk.start()
    get_wv.start()

    @pl.when(jnp.logical_or(z == 0, z == 3))
    def _():
        pl.semaphore_wait(barrier, 3)

    @pl.when(jnp.logical_and(z > 0, z < 3))
    def _():
        pl.semaphore_wait(barrier, 4)

    send_q = pltpu.make_async_remote_copy(q_hbm.at[1 - cc], qbuf.at[cc], qo_s.at[0], qo_r.at[0], device_id=dev_c, device_id_type=MESH)
    got_q = pltpu.make_async_remote_copy(q_hbm.at[1 - cc], qbuf.at[1 - cc], qo_s.at[0], qo_r.at[0], device_id=dev_c, device_id_type=MESH)
    own_y.wait()
    own_a.wait()
    dual(mine, YP).start()
    main(mine, YP).start()
    aux(mine, YP).start()

    @pl.when(z < 3)
    def _():
        full(mine, UP).start()
        aux(mine, UP).start()

    @pl.when(z > 0)
    def _():
        full(mine, DN).start()
        aux(mine, DN).start()

    send_q.start()
    full(mine, CP).start()
    aux(mine, CP).start()

    def relay(i, act):
        to_1 = (UP, DN, DN)[i - 1]
        to_2 = (DN, UP, UP)[i - 1]

        @pl.when(z == 1)
        def _():
            act(to_1)

        @pl.when(z == 2)
        def _():
            act(to_2)

    def event_dual0():
        slot = slot_b(0)
        dual(slot, YP).wait_recv()

        @pl.when(z < 3)
        def _():
            dual(slot, UP).start()

        @pl.when(z > 0)
        def _():
            dual(slot, DN).start()
        dual(slot, CP).start()

    def event_a(i):
        slot = slot_a(i)
        peer = slot_b(i)
        full(slot, UP).wait_recv()
        aux(slot, UP).wait_recv()

        def pass_on(to):
            full(slot, to).start()
            aux(slot, to).start()
        relay(i, pass_on)
        main(slot, YP).start()
        aux(slot, YP).start()
        full(slot, CP).start()
        aux(slot, CP).start()
        dual(peer, UP).wait_recv()
        relay(i, lambda to: dual(peer, to).start())
        dual(peer, CP).start()

    def event_b(i):
        slot = slot_b(i)
        main(slot, YP).wait_recv()
        aux(slot, YP).wait_recv()
        main(slot, CP).start()
        aux(slot, CP).start()

    event_dual0()
    own_q.wait()
    got_q.wait_recv()
    for t in (0, 1):
        for h in range(6):
            q_t[h * 128:(h + 1) * 128, t * 256:(t + 1) * 256] = qbuf[t, :, h * 128:(h + 1) * 128].T
    acc[...] = jnp.zeros_like(acc)
    l_s[...] = jnp.zeros_like(l_s)
    m_s[...] = jnp.full_like(m_s, -jnp.inf)
    get_wk.wait()
    get_wv.wait()
    gain_cols = pl.ds(pl.multiple_of(cc * HALF, 128), HALF)
    bias_k = bk_ref[:, gain_cols].astype(F32)
    gain_k = gk_ref[:, gain_cols].astype(F32)
    bias_v = bv_ref[:, gain_cols].astype(F32)

    def body(it, _):
        last = it // 7
        first = (8 - it) // 8
        is_ac = (it % 2) * (1 - last) + first
        idx = is_ac * ((it + 1) // 2) + (1 - is_ac) * (it // 2 - 1 + last)
        ends = jnp.logical_or(z == 0, z == 3)
        mids = jnp.logical_and(z > 0, z < 3)

        @pl.when(it == 1)
        def _():
            event_a(1)

            @pl.when(mids)
            def _():
                event_a(2)
            event_b(0)

        @pl.when(it == 3)
        def _():
            @pl.when(ends)
            def _():
                event_a(2)

            @pl.when(mids)
            def _():
                event_a(3)
            event_b(1)

        @pl.when(it == 5)
        def _():
            @pl.when(ends)
            def _():
                event_a(3)
            event_b(2)

        @pl.when(it == 7)
        def _():
            event_b(3)

        @pl.when(is_ac == 1)
        def _():
            slot = slot_c(idx)
            full(slot, CP).wait_recv()
            aux(slot, CP).wait_recv()

        @pl.when(is_ac == 0)
        def _():
            slot = slot_d(idx)
            dual(slot, CP).wait_recv()
            main(slot, CP).wait_recv()
            aux(slot, CP).wait_recv()

        y_of = is_ac * yy + (1 - is_ac) * (1 - yy)
        base = z_of(idx) * 4 + y_of * 2
        for s in (0, 1):
            parts = rope_parts(abuf[base + s, 0:128])
            for part in (0, 1):
                rows = pl.ds(s * 256 + part * 128, 128)
                cos_b[rows] = parts[part][0]
                sin_b[rows] = parts[part][1]
                inv_b[rows] = jnp.broadcast_to(abuf[base + s, 128 + part:129 + part], (128, 128)).T
        y_val = ybuf[pl.ds(base, 2)].reshape(2 * TOK, D)
        for hp in range(3):
            wide = slice(hp * 256, (hp + 1) * 256)
            k_lin = jnp.dot(y_val, wk_v[:, wide], preferred_element_type=F32)
            for h2 in (0, 1):
                h_cols = slice((hp * 2 + h2) * 128, (hp * 2 + h2 + 1) * 128)
                val = (k_lin[:, h2 * 128:(h2 + 1) * 128] + bias_k[:, h_cols]) * inv_b[...] * gain_k[:, h_cols]
                k_b[:, h_cols] = (val * cos_b[...] + swap_pairs(val) * sin_b[...]).astype(BF16)
            v_lin = jnp.dot(y_val, wv_v[:, wide], preferred_element_type=F32)
            v_b[:, wide] = (v_lin + bias_v[:, wide]).astype(BF16)
            for h2 in (0, 1):
                h = hp * 2 + h2
                h_cols = slice(h * 128, (h + 1) * 128)
                sc = jnp.dot(k_b[:, h_cols], q_t[h_cols], preferred_element_type=F32)
                m_old = m_s[h]
                m_new = jnp.maximum(m_old, jnp.max(sc, axis=0, keepdims=True) * EXP_SCALE)
                w = jnp.exp2(sc * EXP_SCALE - m_new)
                alpha = jnp.exp2(m_old - m_new)
                l_s[h] = l_s[h] * alpha + jnp.sum(w, axis=0, keepdims=True)
                wv = lax.dot_general(v_b[:, h_cols], w.astype(BF16), (((0,), (0,)), ((), ())), preferred_element_type=F32)
                acc[h] = acc[h] * alpha + wv
                m_s[h] = m_new
        return 0

    lax.fori_loop(0, 8, body, 0)

    for h in range(6):
        o_h = (acc[h] / l_s[h]).T.astype(BF16)
        obuf[0, :, h * 128:(h + 1) * 128] = o_h[:TOK]
        obuf[1, :, h * 128:(h + 1) * 128] = o_h[TOK:]
    send_o = pltpu.make_async_remote_copy(obuf.at[1 - cc], o_hbm.at[cc], qo_s.at[1], qo_r.at[1], device_id=dev_c, device_id_type=MESH)
    got_o = pltpu.make_async_remote_copy(obuf.at[1 - cc], o_hbm.at[1 - cc], qo_s.at[1], qo_r.at[1], device_id=dev_c, device_id_type=MESH)
    keep_o = pltpu.make_async_copy(obuf.at[cc], o_hbm.at[cc], loc.at[5])
    send_o.start()
    keep_o.start()

    dual(mine, YP).wait_send()
    main(mine, YP).wait_send()
    aux(mine, YP).wait_send()
    full(mine, CP).wait_send()
    aux(mine, CP).wait_send()
    dual(slot_b(0), CP).wait_send()

    @pl.when(z < 3)
    def _():
        full(mine, UP).wait_send()
        aux(mine, UP).wait_send()
        dual(slot_b(0), UP).wait_send()

    @pl.when(z > 0)
    def _():
        full(mine, DN).wait_send()
        aux(mine, DN).wait_send()
        dual(slot_b(0), DN).wait_send()

    for i in (1, 2, 3):
        slot = slot_a(i)
        peer = slot_b(i)

        def sent(to, slot=slot, peer=peer):
            full(slot, to).wait_send()
            aux(slot, to).wait_send()
            dual(peer, to).wait_send()
        relay(i, sent)
        main(slot, YP).wait_send()
        aux(slot, YP).wait_send()
        full(slot, CP).wait_send()
        aux(slot, CP).wait_send()
        dual(peer, CP).wait_send()
    for i in range(4):
        main(slot_b(i), CP).wait_send()
        aux(slot_b(i), CP).wait_send()
    send_q.wait_send()
    send_o.wait_send()
    keep_o.wait()
    got_o.wait_recv()


def gather_attention(y, aux, q, wk, wv, bk, gk, bv):
    any_spec = pl.BlockSpec(memory_space=pl.ANY)
    vmem_spec = pl.BlockSpec(memory_space=pltpu.VMEM)
    keys = 16 * TOK
    return pl.pallas_call(
        attn_kernel,
        out_shape=jax.ShapeDtypeStruct((2, TOK, HALF), BF16),
        in_specs=[any_spec] * 5 + [vmem_spec] * 3,
        out_specs=any_spec,
        scratch_shapes=[
            pltpu.VMEM((16, TOK, D), BF16), pltpu.VMEM((16, AUX, 128), F32),
            pltpu.VMEM((2, TOK, HALF), BF16), pltpu.VMEM((HALF, 2 * TOK), BF16),
            pltpu.VMEM((D, HALF), BF16), pltpu.VMEM((D, HALF), BF16),
            pltpu.VMEM((2 * TOK, HALF), BF16), pltpu.VMEM((2 * TOK, HALF), BF16),
            pltpu.VMEM((2 * TOK, 128), F32), pltpu.VMEM((2 * TOK, 128), F32), pltpu.VMEM((2 * TOK, 128), F32),
            pltpu.VMEM((6, HEAD, 2 * TOK), F32), pltpu.VMEM((6, 1, 2 * TOK), F32), pltpu.VMEM((6, 1, 2 * TOK), F32),
            pltpu.VMEM((2, TOK, HALF), BF16),
            pltpu.SemaphoreType.DMA((16,)), pltpu.SemaphoreType.DMA((16,)), pltpu.SemaphoreType.DMA((16,)),
            pltpu.SemaphoreType.DMA((4, 3, 16)), pltpu.SemaphoreType.DMA((6,)),
            pltpu.SemaphoreType.DMA((2,)), pltpu.SemaphoreType.DMA((2,)),
        ],
        cost_estimate=pl.CostEstimate(flops=2 * keys * D * D + 4 * keys * HALF * 2 * TOK, bytes_accessed=4 * D * D, transcendentals=6 * keys * 2 * TOK),
        compiler_params=pltpu.CompilerParams(collective_id=0, has_side_effects=True, vmem_limit_bytes=60 << 20),
        name="gather_attention",
    )(y, aux, q, wk, wv, bk, gk, bv)


def layer_norm(x_f32):
    mean_x = jnp.mean(x_f32, axis=-1, keepdims=True)
    centered = x_f32 - mean_x
    var_x = jnp.mean(centered * centered, axis=-1, keepdims=True)
    return centered * lax.rsqrt(var_x + EPS)


def rms_norm(h_lin, gain):
    return h_lin * lax.rsqrt(jnp.mean(h_lin * h_lin, axis=-1, keepdims=True) + EPS) * gain.astype(jnp.float32)


def project(operand, weight):
    return jnp.dot(operand, weight, preferred_element_type=jnp.float32)


def attention(q_b, k_b, v_b):
    scores = jnp.einsum('bqhd,bkhd->bhqk', q_b, k_b, preferred_element_type=jnp.float32) * (HEAD ** -0.5)
    weights = jnp.exp(scores - jnp.max(scores, axis=-1, keepdims=True))
    weight_sum = jnp.sum(weights, axis=-1)
    weighted_v = jnp.einsum('bhqk,bkhd->bqhd', weights.astype(jnp.bfloat16), v_b, preferred_element_type=jnp.float32)
    return (weighted_v / jnp.transpose(weight_sum, (0, 2, 1))[..., None]).astype(jnp.bfloat16)


def block_tail(x_res, attn_heads, context, ada_mod, attn_wo, attn_bo, norm3_w, norm3_b, cross_wq, cross_wk, cross_wv, cross_gq, cross_gk, cross_wo, ffn_w1, ffn_w2):
    n_batch, n_tok, width = x_res.shape
    n_heads = width // HEAD
    n_text = context.shape[1]
    attn_out = attn_heads.reshape(n_batch, n_tok, width)
    x_one = x_res + ada_mod[:, 2:3] * (project(attn_out, attn_wo) + attn_bo.astype(jnp.float32))
    z_norm = (layer_norm(x_one) * norm3_w.astype(jnp.float32) + norm3_b.astype(jnp.float32)).astype(jnp.bfloat16)
    cross_q = rms_norm(project(z_norm, cross_wq), cross_gq).astype(jnp.bfloat16).reshape(n_batch, n_tok, n_heads, HEAD)
    cross_k = rms_norm(project(context, cross_wk), cross_gk).astype(jnp.bfloat16).reshape(n_batch, n_text, n_heads, HEAD)
    cross_v = project(context, cross_wv).astype(jnp.bfloat16).reshape(n_batch, n_text, n_heads, HEAD)
    cross_out = attention(cross_q, cross_k, cross_v).reshape(n_batch, n_tok, width)
    x_two = x_one + project(cross_out, cross_wo)
    hidden = (layer_norm(x_two) * (1.0 + ada_mod[:, 4:5]) + ada_mod[:, 3:4]).astype(jnp.bfloat16)
    gelu_out = jax.nn.gelu(project(hidden, ffn_w1), approximate=True).astype(jnp.bfloat16)
    return (x_two + ada_mod[:, 5:6] * project(gelu_out, ffn_w2)).astype(jnp.bfloat16)


def solution(mesh):
    tok_spec = P('dp', ('sp', 'uly'), None)
    batch_spec = P('dp', None, None)

    def local_block(tokens, rope_ang, t_emb, block_mod, context, attn_wq, attn_bq, attn_wk, attn_bk, attn_wv, attn_bv, attn_gq, attn_gk, attn_wo, attn_bo, norm3_w, norm3_b, cross_wq, cross_wk, cross_wv, cross_gq, cross_gk, cross_wo, ffn_w1, ffn_w2):
        ada_mod = t_emb + block_mod
        row = lambda vec: vec.reshape(1, -1)
        packed_ang = jnp.concatenate([rope_ang[:128], rope_ang[128:]], axis=1)
        y, q, aux = pre(tokens, t_emb, block_mod, packed_ang, attn_wq, attn_wk, row(attn_bq), row(attn_bk), row(attn_gq))
        o_half = gather_attention(y, aux, q, attn_wk, attn_wv, row(attn_bk), row(attn_gk), row(attn_bv))
        o_tok = jnp.concatenate([o_half[0], o_half[1]], axis=1)[None]
        return block_tail(tokens.astype(jnp.float32), o_tok, context, ada_mod, attn_wo, attn_bo, norm3_w, norm3_b, cross_wq, cross_wk, cross_wv, cross_gq, cross_gk, cross_wo, ffn_w1, ffn_w2)

    in_specs = (tok_spec, P(('sp', 'uly'), None), batch_spec, P(), batch_spec) + (P(),) * 20
    return jax.shard_map(local_block, mesh=mesh, in_specs=in_specs, out_specs=tok_spec, check_vma=False)
```

```python
import math

import jax
import jax.numpy as jnp
from jax import lax
from jax.experimental import pallas as pl
from jax.experimental.pallas import tpu as pltpu
from jax.sharding import PartitionSpec as P

EPS = 1e-6
HEAD = 128
HEADS = 12
D = 1536
FF = 8960
TOK = 256
TEXT = 512
HALF = 768
DUAL = 32
AUX = 136
FT = 1280
RING = 4
MESH = pl.DeviceIdType.MESH
EXP_SCALE = math.log2(math.e) * HEAD ** -0.5
F32 = jnp.float32
BF16 = jnp.bfloat16
VMEM_MAX = 67043328


def dot(lhs, rhs):
    return jnp.dot(lhs, rhs, preferred_element_type=F32)


def dot_dims(lhs, rhs, l_dim, r_dim):
    return lax.dot_general(lhs, rhs, (((l_dim,), (r_dim,)), ((), ())), preferred_element_type=F32)


def swap_pairs(val):
    lane = lax.broadcasted_iota(jnp.int32, val.shape, 1)
    return jnp.where(lane % 2 == 0, pltpu.roll(val, 127, 1), pltpu.roll(val, 1, 1))


def over_pairs(cos_p, sin_p, base):
    lane = lax.broadcasted_iota(jnp.int32, (128, 128), 1)
    sign = jnp.where(lane % 2 == 0, -1.0, 1.0).astype(F32)
    pair = lane // 2 + base
    return jnp.take_along_axis(cos_p, pair, axis=1), jnp.take_along_axis(sin_p, pair, axis=1) * sign


def layer_norm_rows(x_f32):
    centered = x_f32 - jnp.mean(x_f32, axis=-1, keepdims=True)
    var = jnp.mean(centered * centered, axis=-1, keepdims=True)
    return centered * lax.rsqrt(var + EPS)


def fold_sq(val):
    return val[:, :128] * val[:, :128] + val[:, 128:] * val[:, 128:]


def inv_rms(ssq):
    return lax.rsqrt(jnp.sum(ssq, axis=1, keepdims=True) * (1.0 / D) + EPS)


def tile256(j):
    return pl.ds(pl.multiple_of(j * 256, 256), 256)


def tile128(j):
    return pl.ds(pl.multiple_of(j * 128, 128), 128)


def as_row(ref):
    return ref[...].astype(F32).reshape(1, D)


def attn_kernel(x_hbm, ang_hbm, c_hbm, wq_hbm, wk_hbm, wv_hbm, cwk_hbm, cwv_hbm,
                temb_ref, mod_ref, bq_ref, bk_ref, bv_ref, gq_ref, gk_ref, cgk_ref,
                o_hbm, ck_hbm, cvt_hbm,
                xbuf, ang, ctx, wq, wk, wv, cwk, cwv, vec,
                ybuf, abuf, raw, q_loc, q_got, q_t, k_b, v_b, cos_s, sin_s, cos_b, sin_b, inv_b, acc, m_s, l_s,
                craw, ck, cvt, ssq, obuf,
                rs, ss, loc, qo_s, qo_r):
    z = lax.axis_index('sp')
    u = lax.axis_index('uly')
    yy = u // 2
    cc = u % 2
    hi = z // 2
    zm = z * (1 - hi) + (3 - z) * hi
    UP, DN, YP, CP = 0, 1, 2, 3
    dev = ({'sp': (z + 1) % 4, 'uly': u}, {'sp': (z + 3) % 4, 'uly': u},
           {'sp': z, 'uly': (1 - yy) * 2 + cc}, {'sp': z, 'uly': yy * 2 + 1 - cc})
    ends = jnp.logical_or(z == 0, z == 3)
    mids = jnp.logical_and(z > 0, z < 3)

    def z_of(i):
        low = i // 2
        m_i = low * i + (1 - low) * (i + zm - 2 * i * zm)
        return m_i * (1 - hi) + (3 - m_i) * hi

    def slot_a(i):
        return z_of(i) * 4 + yy * 2 + cc

    def slot_b(i):
        return z_of(i) * 4 + (1 - yy) * 2 + cc

    def slot_c(i):
        return z_of(i) * 4 + yy * 2 + 1 - cc

    def slot_d(i):
        return z_of(i) * 4 + (1 - yy) * 2 + 1 - cc

    X1, X2, DU, M1, AX = 'x1', 'x2', 'du', 'm1', 'ax'
    rows_of = {X1: (0, 128), X2: (128, 128), DU: (0, DUAL), M1: (DUAL, 128 - DUAL)}
    sem_of = {X1: 0, M1: 0, X2: 1, DU: 2, AX: 3}

    def copy(slot, part, to):
        ref = abuf.at[slot] if part == AX else ybuf.at[slot, pl.ds(*rows_of[part])]
        key = sem_of[part]
        return pltpu.make_async_remote_copy(ref, ref, ss.at[to, key, slot], rs.at[key, slot], device_id=dev[to], device_id_type=MESH)

    def start(slot, to, *parts):
        for part in parts:
            copy(slot, part, to).start()

    def got(slot, *parts):
        for part in parts:
            copy(slot, part, CP).wait_recv()

    def sent(slot, to, *parts):
        for part in parts:
            copy(slot, part, to).wait_send()

    def along_z(act):
        @pl.when(z < 3)
        def _():
            act(UP)

        @pl.when(z > 0)
        def _():
            act(DN)

    def relay(i, act):
        to_1 = (UP, DN, DN)[i - 1]
        to_2 = (DN, UP, UP)[i - 1]

        @pl.when(z == 1)
        def _():
            act(to_1)

        @pl.when(z == 2)
        def _():
            act(to_2)

    barrier = pltpu.get_barrier_semaphore()
    for to in (YP, CP):
        pl.semaphore_signal(barrier, 1, device_id=dev[to], device_id_type=MESH)
    along_z(lambda to: pl.semaphore_signal(barrier, 1, device_id=dev[to], device_id_type=MESH))

    get_x = pltpu.make_async_copy(x_hbm.at[0], xbuf, loc.at[0])
    get_ang = pltpu.make_async_copy(ang_hbm, ang, loc.at[1])
    get_wk = pltpu.make_async_copy(wk_hbm, wk, loc.at[2])
    get_wq = pltpu.make_async_copy(wq_hbm, wq, loc.at[3])
    get_wv = pltpu.make_async_copy(wv_hbm.at[:, pl.ds(pl.multiple_of(cc * HALF, HALF), HALF)], wv, loc.at[4])
    get_ctx = pltpu.make_async_copy(c_hbm.at[0], ctx, loc.at[5])
    get_cwk = pltpu.make_async_copy(cwk_hbm, cwk, loc.at[6])
    get_cwv = pltpu.make_async_copy(cwv_hbm, cwv, loc.at[7])
    for get in (get_x, get_ang, get_wk, get_wq, get_wv, get_ctx, get_cwk, get_cwv):
        get.start()
    BQ, BK, BV, GQ, GK, CGK = range(6)
    for row, ref in enumerate((bq_ref, bk_ref, bv_ref, gq_ref, gk_ref, cgk_ref)):
        vec[row:row + 1] = as_row(ref)
    shift = temb_ref[0, 0:1] + mod_ref[0, 0:1]
    scale = 1.0 + (temb_ref[0, 1:2] + mod_ref[0, 1:2])
    mine = slot_a(0)
    get_x.wait()

    @pl.loop(0, TOK // 32)
    def _(part):
        rows = pl.ds(pl.multiple_of(part * 32, 32), 32)
        ybuf[mine, rows] = (layer_norm_rows(xbuf[rows].astype(F32)) * scale + shift).astype(BF16)

    @pl.when(ends)
    def _():
        pl.semaphore_wait(barrier, 3)

    @pl.when(mids)
    def _():
        pl.semaphore_wait(barrier, 4)

    start(mine, YP, DU, M1)
    along_z(lambda to: start(mine, to, X1))
    start(mine, CP, X1, X2)

    get_ang.wait()
    abuf[mine, 0:128] = jnp.concatenate([ang[0:128], ang[128:256]], axis=1)
    ssq[0] = jnp.zeros((TOK, 128), F32)
    ssq[1] = jnp.zeros((TOK, 128), F32)
    get_wk.wait()

    @pl.loop(0, 6)
    def _(j):
        ssq[0] += fold_sq(dot(ybuf[mine], wk[:, tile256(j)]) + vec[BK:BK + 1, tile256(j)])
    k_inv = inv_rms(ssq[0])
    for part in (0, 1):
        abuf[mine, 128 + part:129 + part] = jnp.broadcast_to(k_inv[part * 128:(part + 1) * 128], (128, 128)).T[0:1]
    abuf[mine, 130:136] = jnp.zeros((6, 128), F32)
    start(mine, YP, AX, X2)
    along_z(lambda to: start(mine, to, AX, X2))
    start(mine, CP, AX)

    get_wq.wait()

    @pl.loop(0, 6)
    def _(j):
        lin = dot(ybuf[mine], wq[:, tile256(j)]) + vec[BQ:BQ + 1, tile256(j)]
        raw[:, tile256(j)] = lin
        ssq[1] += fold_sq(lin)
    q_inv = inv_rms(ssq[1])
    packed = abuf[mine, 0:128]
    cos_p = jnp.cos(packed)
    sin_p = jnp.sin(packed)
    for part in (0, 1):
        rows = pl.ds(part * 128, 128)
        cos_d, sin_d = over_pairs(cos_p, sin_p, part * 64)
        for h in range(HEADS):
            cols = slice(h * 128, (h + 1) * 128)
            val = raw[rows, cols] * q_inv[part * 128:(part + 1) * 128] * vec[GQ:GQ + 1, cols]
            q_loc[h // 6, rows, (h % 6) * 128:(h % 6 + 1) * 128] = (val * cos_d + swap_pairs(val) * sin_d).astype(BF16)
    send_q = pltpu.make_async_remote_copy(q_loc.at[1 - cc], q_got, qo_s.at[0], qo_r.at[0], device_id=dev[CP], device_id_type=MESH)
    send_q.start()

    peer0 = slot_b(0)
    got(peer0, DU)
    along_z(lambda to: start(peer0, to, DU))
    start(peer0, CP, DU)

    def event_a(i, hf):
        slot = slot_a(i)
        peer = slot_b(i)
        if hf:
            got(slot, X2)
            relay(i, lambda to: start(slot, to, X2))
            start(slot, YP, X2)
            start(slot, CP, X2)
        else:
            got(slot, X1, AX)
            relay(i, lambda to: start(slot, to, X1, AX))
            start(slot, YP, M1, AX)
            start(slot, CP, X1, AX)
            got(peer, DU)
            relay(i, lambda to: start(peer, to, DU))
            start(peer, CP, DU)

    def event_b(i, hf):
        slot = slot_b(i)
        parts = (X2,) if hf else (M1, AX)
        got(slot, *parts)
        start(slot, CP, *parts)

    for h in range(6):
        cols = slice(h * 128, (h + 1) * 128)
        q_t[cols, pl.ds(pl.multiple_of(cc * TOK, TOK), TOK)] = q_loc[cc, :, cols].T
    acc[...] = jnp.zeros_like(acc)
    l_s[...] = jnp.zeros_like(l_s)
    m_s[...] = jnp.full_like(m_s, -jnp.inf)
    send_q.wait_recv()
    for h in range(6):
        cols = slice(h * 128, (h + 1) * 128)
        q_t[cols, pl.ds(pl.multiple_of((1 - cc) * TOK, TOK), TOK)] = q_got[:, cols].T
    get_wv.wait()

    def cross_k():
        get_ctx.wait()
        get_cwk.wait()
        ssq[...] = jnp.zeros_like(ssq)

        @pl.loop(0, 6)
        def _(j):
            lin = dot(ctx[...], cwk[:, tile256(j)])
            craw[:, tile256(j)] = lin
            sq = fold_sq(lin)
            ssq[0] += sq[:TOK]
            ssq[1] += sq[TOK:]
        inv_0 = inv_rms(ssq[0])
        inv_1 = inv_rms(ssq[1])

        @pl.loop(0, 6)
        def _(j):
            gain = vec[CGK:CGK + 1, tile256(j)]
            ck[0:TOK, tile256(j)] = (craw[0:TOK, tile256(j)] * inv_0 * gain).astype(BF16)
            ck[TOK:TEXT, tile256(j)] = (craw[TOK:TEXT, tile256(j)] * inv_1 * gain).astype(BF16)
        pltpu.make_async_copy(ck, ck_hbm, loc.at[8]).start()

    def cross_v():
        get_cwv.wait()

        @pl.loop(0, 6)
        def _(j):
            cvt[tile256(j), :] = dot(ctx[...], cwv[:, tile256(j)]).astype(BF16).T
        pltpu.make_async_copy(cvt, cvt_hbm, loc.at[9]).start()

    at_ends = {2: ('a', 1, 0), 4: ('a', 1, 1), 6: ('a', 2, 0), 8: ('a', 2, 1), 10: ('a', 3, 0), 12: ('a', 3, 1)}
    at_mids = {2: ('a', 1, 0, 2, 0), 4: ('a', 1, 1, 2, 1), 8: ('a', 3, 0), 10: ('a', 3, 1)}
    at_all = {3: (0, 0), 5: (0, 1), 7: (1, 0), 9: (1, 1), 11: (2, 0), 13: (2, 1), 14: (3, 0), 15: (3, 1)}

    def body(it, _):
        first = (15 - it) // 14
        last = it // 14
        mid = 1 - first - last
        r = (it + 2) % 4
        k = (it + 2) // 4 - 1
        is_bd = mid * (r % 2) + last
        hf = mid * (r // 2) + (first + last) * (it % 2)
        idx = mid * (k + 1 - r % 2) + last * 3

        for step in range(16):
            has_ends, has_mids, has_all = step in at_ends, step in at_mids, step in at_all
            if not (has_ends or has_mids or has_all):
                continue

            @pl.when(it == step)
            def _(step=step, has_ends=has_ends, has_mids=has_mids, has_all=has_all):
                if has_ends:
                    @pl.when(ends)
                    def _():
                        event_a(*at_ends[step][1:3])
                if has_mids:
                    @pl.when(mids)
                    def _():
                        todo = at_mids[step][1:]
                        for n in range(0, len(todo), 2):
                            event_a(todo[n], todo[n + 1])
                if has_all:
                    event_b(*at_all[step])

        pl.when(it == 4)(cross_k)
        pl.when(it == 8)(cross_v)

        @pl.when(jnp.logical_and(is_bd == 0, hf == 0))
        def _():
            got(slot_c(idx), X1, AX)

        @pl.when(jnp.logical_and(is_bd == 0, hf == 1))
        def _():
            got(slot_c(idx), X2)

        @pl.when(jnp.logical_and(is_bd == 1, hf == 0))
        def _():
            got(slot_d(idx), DU, M1, AX)

        @pl.when(jnp.logical_and(is_bd == 1, hf == 1))
        def _():
            got(slot_d(idx), X2)

        y_of = (1 - is_bd) * yy + is_bd * (1 - yy)
        base = z_of(idx) * 4 + y_of * 2

        @pl.when(hf == 0)
        def _():
            for s in (0, 1):
                packed = abuf[base + s, 0:128]
                cos_s[is_bd * 2 + s] = jnp.cos(packed)
                sin_s[is_bd * 2 + s] = jnp.sin(packed)
        for s in (0, 1):
            rows = slice(s * 128, (s + 1) * 128)
            cos_b[rows], sin_b[rows] = over_pairs(cos_s[is_bd * 2 + s], sin_s[is_bd * 2 + s], hf * 64)
            inv_b[rows] = jnp.broadcast_to(abuf[base + s, pl.ds(128 + hf, 1)], (128, 128)).T
        y_val = ybuf[pl.ds(base, 2), pl.ds(pl.multiple_of(hf * 128, 128), 128)].reshape(TOK, D)
        for hp in range(3):
            wide = slice(hp * 256, (hp + 1) * 256)
            mine_cols = pl.ds(pl.multiple_of(cc * HALF + hp * 256, 256), 256)
            k_lin = dot(y_val, wk[:, mine_cols]) + vec[BK:BK + 1, mine_cols]
            gain = vec[GK:GK + 1, mine_cols]
            for h2 in (0, 1):
                cols = slice(h2 * 128, (h2 + 1) * 128)
                val = k_lin[:, cols] * inv_b[...] * gain[:, cols]
                k_b[:, (hp * 2 + h2) * 128:(hp * 2 + h2 + 1) * 128] = (val * cos_b[...] + swap_pairs(val) * sin_b[...]).astype(BF16)
            v_b[:, wide] = (dot(y_val, wv[:, wide]) + vec[BV:BV + 1, mine_cols]).astype(BF16)
            for h2 in (0, 1):
                h = hp * 2 + h2
                cols = slice(h * 128, (h + 1) * 128)
                sc = dot(k_b[:, cols], q_t[cols])
                m_old = m_s[h]
                m_new = jnp.maximum(m_old, jnp.max(sc, axis=0, keepdims=True) * EXP_SCALE)
                w = jnp.exp2(sc * EXP_SCALE - m_new)
                alpha = jnp.exp2(m_old - m_new)
                l_s[h] = l_s[h] * alpha + jnp.sum(w, axis=0, keepdims=True)
                acc[h] = acc[h] * alpha + dot_dims(v_b[:, cols], w.astype(BF16), 0, 0)
                m_s[h] = m_new
        return 0

    lax.fori_loop(0, 16, body, 0)

    for h in range(6):
        cols = slice(h * 128, (h + 1) * 128)
        o_h = (acc[h] / l_s[h]).T.astype(BF16)
        obuf[0, :, cols] = o_h[:TOK]
        obuf[1, :, cols] = o_h[TOK:]
    send_o = pltpu.make_async_remote_copy(obuf.at[1 - cc], o_hbm.at[cc], qo_s.at[1], qo_r.at[1], device_id=dev[CP], device_id_type=MESH)
    got_o = pltpu.make_async_remote_copy(obuf.at[1 - cc], o_hbm.at[1 - cc], qo_s.at[1], qo_r.at[1], device_id=dev[CP], device_id_type=MESH)
    keep_o = pltpu.make_async_copy(obuf.at[cc], o_hbm.at[cc], loc.at[10])
    send_o.start()
    keep_o.start()

    sent(mine, YP, DU, M1, AX, X2)
    sent(mine, CP, X1, X2, AX)
    sent(peer0, CP, DU)

    def sent_z(to):
        sent(mine, to, X1, AX, X2)
        sent(peer0, to, DU)
    along_z(sent_z)
    for i in (1, 2, 3):
        slot = slot_a(i)
        peer = slot_b(i)

        def sent_on(to, slot=slot, peer=peer):
            sent(slot, to, X1, AX, X2)
            sent(peer, to, DU)
        relay(i, sent_on)
        sent(slot, YP, M1, AX, X2)
        sent(slot, CP, X1, AX, X2)
        sent(peer, CP, DU)
    for i in range(4):
        sent(slot_b(i), CP, M1, AX, X2)
    send_q.wait_send()
    pltpu.make_async_copy(ck, ck_hbm, loc.at[8]).wait()
    pltpu.make_async_copy(cvt, cvt_hbm, loc.at[9]).wait()
    send_o.wait_send()
    keep_o.wait()
    got_o.wait_recv()


def gather_attention(*args):
    any_spec = pl.BlockSpec(memory_space=pl.ANY)
    vmem_spec = pl.BlockSpec(memory_space=pltpu.VMEM)
    keys = 16 * TOK
    square = pltpu.VMEM((D, D), BF16)
    return pl.pallas_call(
        attn_kernel,
        out_shape=[jax.ShapeDtypeStruct((2, TOK, HALF), BF16), jax.ShapeDtypeStruct((TEXT, D), BF16), jax.ShapeDtypeStruct((D, TEXT), BF16)],
        in_specs=[any_spec] * 8 + [vmem_spec] * 8,
        out_specs=[any_spec] * 3,
        scratch_shapes=[
            pltpu.VMEM((TOK, D), BF16), pltpu.VMEM((TOK, 64), F32), pltpu.VMEM((TEXT, D), BF16),
            square, square, pltpu.VMEM((D, HALF), BF16), square, square, pltpu.VMEM((8, D), F32),
            pltpu.VMEM((16, TOK, D), BF16), pltpu.VMEM((16, AUX, 128), F32), pltpu.VMEM((TOK, D), F32),
            pltpu.VMEM((2, TOK, HALF), BF16), pltpu.VMEM((TOK, HALF), BF16), pltpu.VMEM((HALF, 2 * TOK), BF16),
            pltpu.VMEM((TOK, HALF), BF16), pltpu.VMEM((TOK, HALF), BF16),
            pltpu.VMEM((4, 128, 128), F32), pltpu.VMEM((4, 128, 128), F32),
            pltpu.VMEM((TOK, 128), F32), pltpu.VMEM((TOK, 128), F32), pltpu.VMEM((TOK, 128), F32),
            pltpu.VMEM((6, HEAD, 2 * TOK), F32), pltpu.VMEM((6, 1, 2 * TOK), F32), pltpu.VMEM((6, 1, 2 * TOK), F32),
            pltpu.VMEM((TEXT, D), F32), pltpu.VMEM((TEXT, D), BF16), pltpu.VMEM((D, TEXT), BF16), pltpu.VMEM((2, TOK, 128), F32),
            pltpu.VMEM((2, TOK, HALF), BF16),
            pltpu.SemaphoreType.DMA((4, 16)), pltpu.SemaphoreType.DMA((4, 4, 16)), pltpu.SemaphoreType.DMA((11,)),
            pltpu.SemaphoreType.DMA((2,)), pltpu.SemaphoreType.DMA((2,)),
        ],
        cost_estimate=pl.CostEstimate(flops=2 * keys * D * D + 4 * keys * HALF * 2 * TOK, bytes_accessed=10 * D * D, transcendentals=6 * keys * 2 * TOK),
        compiler_params=pltpu.CompilerParams(collective_id=0, has_side_effects=True, vmem_limit_bytes=VMEM_MAX),
        name="gather_attention",
    )(*args)


def tail_kernel(o_hbm, x_hbm, ck_hbm, cvt_hbm, wo_hbm, cwq_hbm, cwo_hbm, w1_hbm, w2_hbm,
                temb_ref, mod_ref, bo_ref, nw_ref, nb_ref, cgq_ref, out_ref,
                o_v, x_v, ck, cvt, wo, cwq, cwo, w1, w2, vec, res, lin, act, u_b, ssq, sems, ring):
    n_ff = FF // FT

    def ff_copies(t, slot):
        cols = pl.ds(pl.multiple_of(t * FT, FT), FT)
        return (pltpu.make_async_copy(w1_hbm.at[:, cols], w1.at[slot], ring.at[0, slot]),
                pltpu.make_async_copy(w2_hbm.at[cols], w2.at[slot], ring.at[1, slot]))

    gets = [pltpu.make_async_copy(src, dst, sems.at[n]) for n, (src, dst) in enumerate(
        ((o_hbm, o_v), (wo_hbm, wo), (x_hbm.at[0], x_v), (cwq_hbm, cwq), (ck_hbm, ck), (cvt_hbm, cvt), (cwo_hbm, cwo)))]
    for get in gets:
        get.start()
    for t in range(RING):
        for get in ff_copies(t, t):
            get.start()
    get_o, get_wo, get_x, get_cwq, get_ck, get_cvt, get_cwo = gets
    vec[0:6] = temb_ref[0] + mod_ref[0]
    BO, NW, NB, CGQ = 6, 7, 8, 9
    for row, ref in ((BO, bo_ref), (NW, nw_ref), (NB, nb_ref), (CGQ, cgq_ref)):
        vec[row:row + 1] = as_row(ref)

    get_o.wait()
    get_wo.wait()
    get_x.wait()

    @pl.loop(0, 6)
    def _(j):
        cols = tile256(j)
        prod = dot(o_v[0], wo[0:HALF, cols]) + dot(o_v[1], wo[HALF:D, cols])
        res[:, cols] = x_v[:, cols].astype(F32) + vec[2:3, cols] * (prod + vec[BO:BO + 1, cols])

    @pl.loop(0, TOK // 32)
    def _(part):
        rows = pl.ds(pl.multiple_of(part * 32, 32), 32)
        act[rows] = (layer_norm_rows(res[rows]) * vec[NW:NW + 1] + vec[NB:NB + 1]).astype(BF16)
    get_cwq.wait()
    ssq[...] = jnp.zeros_like(ssq)

    @pl.loop(0, 6)
    def _(j):
        prod = dot(act[...], cwq[:, tile256(j)])
        lin[:, tile256(j)] = prod
        ssq[...] += fold_sq(prod)
    q_inv = inv_rms(ssq[...])
    get_ck.wait()
    get_cvt.wait()

    @pl.loop(0, HEADS // 2)
    def _(hp):
        for h2 in (0, 1):
            cols = tile128(hp * 2 + h2)
            q_h = (lin[:, cols] * q_inv * vec[CGQ:CGQ + 1, cols]).astype(BF16)
            sc = dot_dims(ck[:, cols], q_h, 1, 1)
            m_row = jnp.max(sc, axis=0, keepdims=True) * EXP_SCALE
            w = jnp.exp2(sc * EXP_SCALE - m_row)
            o_t = dot(cvt[cols, :], w.astype(BF16)) / jnp.sum(w, axis=0, keepdims=True)
            act[:, cols] = o_t.T.astype(BF16)
    get_cwo.wait()

    @pl.loop(0, 6)
    def _(j):
        cols = tile256(j)
        res[:, cols] += dot(act[...], cwo[:, cols])

    @pl.loop(0, TOK // 32)
    def _(part):
        rows = pl.ds(pl.multiple_of(part * 32, 32), 32)
        act[rows] = (layer_norm_rows(res[rows]) * (1.0 + vec[4:5]) + vec[3:4]).astype(BF16)
        lin[rows] = jnp.zeros((32, D), F32)

    def ffn(t, _):
        slot = t % RING
        for get in ff_copies(t, slot):
            get.wait()
        for s in range(FT // 256):
            cols = slice(s * 256, (s + 1) * 256)
            u_b[:, cols] = jax.nn.gelu(dot(act[...], w1[slot, :, cols]), approximate=True).astype(BF16)
        for j in range(6):
            cols = slice(j * 256, (j + 1) * 256)
            lin[:, cols] += dot(u_b[...], w2[slot, :, cols])

        @pl.when(t + RING < n_ff)
        def _():
            for get in ff_copies(t + RING, slot):
                get.start()
        return 0

    lax.fori_loop(0, n_ff, ffn, 0)

    @pl.loop(0, TOK // 32)
    def _(part):
        rows = pl.ds(pl.multiple_of(part * 32, 32), 32)
        out_ref[0, rows] = (res[rows] + vec[5:6] * lin[rows]).astype(BF16)


def tail(*args):
    any_spec = pl.BlockSpec(memory_space=pl.ANY)
    vmem_spec = pl.BlockSpec(memory_space=pltpu.VMEM)
    square = pltpu.VMEM((D, D), BF16)
    return pl.pallas_call(
        tail_kernel,
        out_shape=jax.ShapeDtypeStruct((1, TOK, D), BF16),
        in_specs=[any_spec] * 9 + [vmem_spec] * 6,
        out_specs=vmem_spec,
        scratch_shapes=[
            pltpu.VMEM((2, TOK, HALF), BF16), pltpu.VMEM((TOK, D), BF16), pltpu.VMEM((TEXT, D), BF16), pltpu.VMEM((D, TEXT), BF16),
            square, square, square, pltpu.VMEM((RING, D, FT), BF16), pltpu.VMEM((RING, FT, D), BF16), pltpu.VMEM((16, D), F32),
            pltpu.VMEM((TOK, D), F32), pltpu.VMEM((TOK, D), F32), pltpu.VMEM((TOK, D), BF16), pltpu.VMEM((TOK, FT), BF16), pltpu.VMEM((TOK, 128), F32),
            pltpu.SemaphoreType.DMA((7,)), pltpu.SemaphoreType.DMA((2, RING)),
        ],
        cost_estimate=pl.CostEstimate(flops=4 * TOK * D * FF + 6 * TOK * D * D, bytes_accessed=4 * D * FF + 6 * D * D, transcendentals=TOK * FF),
        compiler_params=pltpu.CompilerParams(vmem_limit_bytes=VMEM_MAX),
        name="tail",
    )(*args)


def solution(mesh):
    tok_spec = P('dp', ('sp', 'uly'), None)
    batch_spec = P('dp', None, None)

    def local_block(tokens, rope_ang, t_emb, block_mod, context, attn_wq, attn_bq, attn_wk, attn_bk, attn_wv, attn_bv, attn_gq, attn_gk, attn_wo, attn_bo, norm3_w, norm3_b, cross_wq, cross_wk, cross_wv, cross_gq, cross_gk, cross_wo, ffn_w1, ffn_w2):
        o_half, cross_k, cross_vt = gather_attention(tokens, rope_ang, context, attn_wq, attn_wk, attn_wv, cross_wk, cross_wv, t_emb, block_mod, attn_bq, attn_bk, attn_bv, attn_gq, attn_gk, cross_gk)
        return tail(o_half, tokens, cross_k, cross_vt, attn_wo, cross_wq, cross_wo, ffn_w1, ffn_w2, t_emb, block_mod, attn_bo, norm3_w, norm3_b, cross_gq)

    in_specs = (tok_spec, P(('sp', 'uly'), None), batch_spec, P(), batch_spec) + (P(),) * 20
    return jax.shard_map(local_block, mesh=mesh, in_specs=in_specs, out_specs=tok_spec, check_vma=False)
```

```python
import math

import jax
import jax.numpy as jnp
from jax import lax
from jax.experimental import pallas as pl
from jax.experimental.pallas import tpu as pltpu
from jax.sharding import PartitionSpec as P

EPS = 1e-6
HEAD = 128
LANES = 128
HEADS = 12
D = 1536
FF = 8960
TOK = 256
WIDE = 256
TEXT = 512
HALF = 768
DUAL = 32
AUX = 136
FT = 1280
RING = 4
MESH = pl.DeviceIdType.MESH
EXP_SCALE = math.log2(math.e) * HEAD ** -0.5
F32 = jnp.float32
BF16 = jnp.bfloat16
VMEM_MAX = 67043328


def dot(lhs, rhs):
    return jnp.dot(lhs, rhs, preferred_element_type=F32)


def dot_dims(lhs, rhs, l_dim, r_dim):
    return lax.dot_general(lhs, rhs, (((l_dim,), (r_dim,)), ((), ())), preferred_element_type=F32)


def swap_pairs(val):
    lane = lax.broadcasted_iota(jnp.int32, val.shape, 1)
    return jnp.where(lane % 2 == 0, pltpu.roll(val, 127, 1), pltpu.roll(val, 1, 1))


def over_pairs(cos_p, sin_p, base):
    lane = lax.broadcasted_iota(jnp.int32, (LANES, LANES), 1)
    sign = jnp.where(lane % 2 == 0, -1.0, 1.0).astype(F32)
    pair = lane // 2 + base
    return jnp.take_along_axis(cos_p, pair, axis=1), jnp.take_along_axis(sin_p, pair, axis=1) * sign


def layer_norm_rows(x_f32):
    centered = x_f32 - jnp.mean(x_f32, axis=-1, keepdims=True)
    var = jnp.mean(centered * centered, axis=-1, keepdims=True)
    return centered * lax.rsqrt(var + EPS)


def fold_sq(val):
    return val[:, :LANES] * val[:, :LANES] + val[:, LANES:] * val[:, LANES:]


def inv_rms(ssq):
    return lax.rsqrt(jnp.sum(ssq, axis=1, keepdims=True) * (1.0 / D) + EPS)


def tile256(j):
    return pl.ds(pl.multiple_of(j * WIDE, WIDE), WIDE)


def tile128(j):
    return pl.ds(pl.multiple_of(j * LANES, LANES), LANES)


def ada_row(temb_ref, mod_ref, row):
    cols = slice(row * D, (row + 1) * D)
    return (temb_ref[cols] + mod_ref[cols]).reshape(1, D)


def as_row(ref):
    return ref[...].astype(F32).reshape(1, D)


def attn_kernel(x_hbm, ang_hbm, c_hbm, wq_hbm, wk_hbm, wv_hbm, cwk_hbm, cwv_hbm,
                temb_ref, mod_ref, bq_ref, bk_ref, bv_ref, gq_ref, gk_ref, cgk_ref,
                o_hbm, ck_hbm, cvt_hbm,
                xbuf, ang, ctx, wq, wk, wv, cwk, cwv, vec,
                ybuf, abuf, raw, q_loc, q_got, q_t, k_b, v_b, cos_s, sin_s, cos_b, sin_b, inv_b, acc, m_s, l_s, k_f, sc_s, w_s,
                craw, ck, cvt, ssq, obuf,
                rs, ss, loc, qo_s, qo_r):
    z = lax.axis_index('sp')
    u = lax.axis_index('uly')
    yy = u // 2
    cc = u % 2
    hi = z // 2
    zm = z * (1 - hi) + (3 - z) * hi
    UP, DN, YP, CP = 0, 1, 2, 3
    dev = ({'sp': (z + 1) % 4, 'uly': u}, {'sp': (z + 3) % 4, 'uly': u},
           {'sp': z, 'uly': (1 - yy) * 2 + cc}, {'sp': z, 'uly': yy * 2 + 1 - cc})
    ends = jnp.logical_or(z == 0, z == 3)
    mids = jnp.logical_and(z > 0, z < 3)

    def z_of(i):
        low = i // 2
        m_i = low * i + (1 - low) * (i + zm - 2 * i * zm)
        return m_i * (1 - hi) + (3 - m_i) * hi

    def slot_a(i):
        return z_of(i) * 4 + yy * 2 + cc

    def slot_b(i):
        return z_of(i) * 4 + (1 - yy) * 2 + cc

    def slot_c(i):
        return z_of(i) * 4 + yy * 2 + 1 - cc

    def slot_d(i):
        return z_of(i) * 4 + (1 - yy) * 2 + 1 - cc

    X1, X2, DU, M1, AX = 'x1', 'x2', 'du', 'm1', 'ax'
    rows_of = {X1: (0, LANES), X2: (LANES, LANES), DU: (0, DUAL), M1: (DUAL, LANES - DUAL)}
    sem_of = {X1: 0, M1: 0, X2: 1, DU: 2, AX: 3}

    def copy(slot, part, to):
        ref = abuf.at[slot] if part == AX else ybuf.at[slot, pl.ds(*rows_of[part])]
        key = sem_of[part]
        return pltpu.make_async_remote_copy(ref, ref, ss.at[to, key, slot], rs.at[key, slot], device_id=dev[to], device_id_type=MESH)

    def start(slot, to, *parts):
        for part in parts:
            copy(slot, part, to).start()

    def got(slot, *parts):
        for part in parts:
            copy(slot, part, CP).wait_recv()

    def sent(slot, to, *parts):
        for part in parts:
            copy(slot, part, to).wait_send()

    def along_z(act):
        @pl.when(z < 3)
        def _():
            act(UP)

        @pl.when(z > 0)
        def _():
            act(DN)

    def relay(i, act):
        to_1 = (UP, DN, DN)[i - 1]
        to_2 = (DN, UP, UP)[i - 1]

        @pl.when(z == 1)
        def _():
            act(to_1)

        @pl.when(z == 2)
        def _():
            act(to_2)

    barrier = pltpu.get_barrier_semaphore()
    for to in (YP, CP):
        pl.semaphore_signal(barrier, 1, device_id=dev[to], device_id_type=MESH)
    along_z(lambda to: pl.semaphore_signal(barrier, 1, device_id=dev[to], device_id_type=MESH))

    get_x = pltpu.make_async_copy(x_hbm.at[0], xbuf, loc.at[0])
    get_ang = pltpu.make_async_copy(ang_hbm, ang, loc.at[1])
    get_wk = pltpu.make_async_copy(wk_hbm, wk, loc.at[2])
    get_wq = pltpu.make_async_copy(wq_hbm, wq, loc.at[3])
    get_wv = pltpu.make_async_copy(wv_hbm.at[:, pl.ds(pl.multiple_of(cc * HALF, HALF), HALF)], wv, loc.at[4])
    get_ctx = pltpu.make_async_copy(c_hbm.at[0], ctx, loc.at[5])
    get_cwk = pltpu.make_async_copy(cwk_hbm, cwk, loc.at[6])
    get_cwv = pltpu.make_async_copy(cwv_hbm, cwv, loc.at[7])
    for get in (get_x, get_ang, get_wk):
        get.start()
    BQ, BK, BV, GQ, GK, CGK = range(6)
    for row, ref in enumerate((bq_ref, bk_ref, bv_ref, gq_ref, gk_ref, cgk_ref)):
        vec[row:row + 1] = as_row(ref)
    shift = ada_row(temb_ref, mod_ref, 0)
    scale = 1.0 + ada_row(temb_ref, mod_ref, 1)
    mine = slot_a(0)
    get_x.wait()
    get_wq.start()

    @pl.loop(0, TOK // 32)
    def _(part):
        rows = pl.ds(pl.multiple_of(part * 32, 32), 32)
        ybuf[mine, rows] = (layer_norm_rows(xbuf[rows].astype(F32)) * scale + shift).astype(BF16)

    @pl.when(ends)
    def _():
        pl.semaphore_wait(barrier, 3)

    @pl.when(mids)
    def _():
        pl.semaphore_wait(barrier, 4)

    start(mine, YP, DU, M1)
    along_z(lambda to: start(mine, to, X1))
    start(mine, CP, X1, X2)

    get_ang.wait()
    abuf[mine, 0:LANES] = jnp.concatenate([ang[:, 0:LANES], ang[:, LANES:WIDE]], axis=0).T
    ssq[0] = jnp.zeros((TOK, LANES), F32)
    ssq[1] = jnp.zeros((TOK, LANES), F32)
    get_wk.wait()
    for get in (get_wv, get_ctx, get_cwk, get_cwv):
        get.start()

    @pl.loop(0, 6)
    def _(j):
        ssq[0] += fold_sq(dot(ybuf[mine], wk[:, tile256(j)]) + vec[BK:BK + 1, tile256(j)])
    k_inv = inv_rms(ssq[0])
    for part in (0, 1):
        abuf[mine, LANES + part:129 + part] = jnp.broadcast_to(k_inv[part * LANES:(part + 1) * LANES], (LANES, LANES)).T[0:1]
    abuf[mine, 130:136] = jnp.zeros((6, LANES), F32)
    start(mine, YP, AX, X2)
    along_z(lambda to: start(mine, to, AX, X2))
    start(mine, CP, AX)

    get_wq.wait()

    @pl.loop(0, 6)
    def _(j):
        lin = dot(ybuf[mine], wq[:, tile256(j)]) + vec[BQ:BQ + 1, tile256(j)]
        raw[:, tile256(j)] = lin
        ssq[1] += fold_sq(lin)
    q_inv = inv_rms(ssq[1])
    packed = abuf[mine, 0:LANES]
    cos_p = jnp.cos(packed)
    sin_p = jnp.sin(packed)
    for part in (0, 1):
        rows = pl.ds(part * LANES, LANES)
        cos_d, sin_d = over_pairs(cos_p, sin_p, part * 64)
        for h in range(HEADS):
            cols = slice(h * LANES, (h + 1) * LANES)
            val = raw[rows, cols] * q_inv[part * LANES:(part + 1) * LANES] * vec[GQ:GQ + 1, cols]
            q_loc[h // 6, rows, (h % 6) * LANES:(h % 6 + 1) * LANES] = (val * cos_d + swap_pairs(val) * sin_d).astype(BF16)
    send_q = pltpu.make_async_remote_copy(q_loc.at[1 - cc], q_got, qo_s.at[0], qo_r.at[0], device_id=dev[CP], device_id_type=MESH)
    send_q.start()

    peer0 = slot_b(0)
    got(peer0, DU)
    along_z(lambda to: start(peer0, to, DU))
    start(peer0, CP, DU)

    def event_a(i, hf):
        slot = slot_a(i)
        peer = slot_b(i)
        if hf:
            got(slot, X2)
            relay(i, lambda to: start(slot, to, X2))
            start(slot, YP, X2)
            start(slot, CP, X2)
        else:
            got(slot, X1, AX)
            relay(i, lambda to: start(slot, to, X1, AX))
            start(slot, YP, M1, AX)
            start(slot, CP, X1, AX)
            got(peer, DU)
            relay(i, lambda to: start(peer, to, DU))
            start(peer, CP, DU)

    def event_b(i, hf):
        slot = slot_b(i)
        parts = (X2,) if hf else (M1, AX)
        got(slot, *parts)
        start(slot, CP, *parts)

    for h in range(6):
        cols = slice(h * LANES, (h + 1) * LANES)
        q_t[cols, pl.ds(pl.multiple_of(cc * TOK, TOK), TOK)] = q_loc[cc, :, cols].T
    acc[...] = jnp.zeros_like(acc)
    l_s[...] = jnp.zeros_like(l_s)
    m_s[...] = jnp.full_like(m_s, -jnp.inf)
    send_q.wait_recv()
    for h in range(6):
        cols = slice(h * LANES, (h + 1) * LANES)
        q_t[cols, pl.ds(pl.multiple_of((1 - cc) * TOK, TOK), TOK)] = q_got[:, cols].T
    get_wv.wait()

    def cross_k():
        get_ctx.wait()
        get_cwk.wait()
        ssq[...] = jnp.zeros_like(ssq)

        @pl.loop(0, 6)
        def _(j):
            lin = dot(ctx[...], cwk[:, tile256(j)])
            craw[:, tile256(j)] = lin
            sq = fold_sq(lin)
            ssq[0] += sq[:TOK]
            ssq[1] += sq[TOK:]
        inv_0 = inv_rms(ssq[0])
        inv_1 = inv_rms(ssq[1])

        @pl.loop(0, 6)
        def _(j):
            gain = vec[CGK:CGK + 1, tile256(j)]
            ck[0:TOK, tile256(j)] = (craw[0:TOK, tile256(j)] * inv_0 * gain).astype(BF16)
            ck[TOK:TEXT, tile256(j)] = (craw[TOK:TEXT, tile256(j)] * inv_1 * gain).astype(BF16)
        pltpu.make_async_copy(ck, ck_hbm, loc.at[8]).start()

    def cross_v():
        get_cwv.wait()

        @pl.loop(0, 6)
        def _(j):
            cvt[tile256(j), :] = dot(ctx[...], cwv[:, tile256(j)]).astype(BF16).T
        pltpu.make_async_copy(cvt, cvt_hbm, loc.at[9]).start()

    at_ends = {2: ('a', 1, 0), 4: ('a', 1, 1), 6: ('a', 2, 0), 8: ('a', 2, 1), 10: ('a', 3, 0), 12: ('a', 3, 1)}
    at_mids = {2: ('a', 1, 0, 2, 0), 4: ('a', 1, 1, 2, 1), 8: ('a', 3, 0), 10: ('a', 3, 1)}
    at_all = {3: (0, 0), 5: (0, 1), 7: (1, 0), 9: (1, 1), 11: (2, 0), 13: (2, 1), 14: (3, 0), 15: (3, 1)}

    def body(it, _):
        first = (15 - it) // 14
        last = it // 14
        mid = 1 - first - last
        r = (it + 2) % 4
        k = (it + 2) // 4 - 1
        is_bd = mid * (r % 2) + last
        hf = mid * (r // 2) + (first + last) * (it % 2)
        idx = mid * (k + 1 - r % 2) + last * 3

        for step in range(16):
            has_ends, has_mids, has_all = step in at_ends, step in at_mids, step in at_all
            if not (has_ends or has_mids or has_all):
                continue

            @pl.when(it == step)
            def _(step=step, has_ends=has_ends, has_mids=has_mids, has_all=has_all):
                if has_ends:
                    @pl.when(ends)
                    def _():
                        event_a(*at_ends[step][1:3])
                if has_mids:
                    @pl.when(mids)
                    def _():
                        todo = at_mids[step][1:]
                        for n in range(0, len(todo), 2):
                            event_a(todo[n], todo[n + 1])
                if has_all:
                    event_b(*at_all[step])

        pl.when(it == 4)(cross_k)
        pl.when(it == 8)(cross_v)

        @pl.when(jnp.logical_and(is_bd == 0, hf == 0))
        def _():
            got(slot_c(idx), X1, AX)

        @pl.when(jnp.logical_and(is_bd == 0, hf == 1))
        def _():
            got(slot_c(idx), X2)

        @pl.when(jnp.logical_and(is_bd == 1, hf == 0))
        def _():
            got(slot_d(idx), DU, M1, AX)

        @pl.when(jnp.logical_and(is_bd == 1, hf == 1))
        def _():
            got(slot_d(idx), X2)

        y_of = (1 - is_bd) * yy + is_bd * (1 - yy)
        base = z_of(idx) * 4 + y_of * 2

        @pl.when(hf == 0)
        def _():
            for s in (0, 1):
                packed = abuf[base + s, 0:LANES]
                cos_s[is_bd * 2 + s] = jnp.cos(packed)
                sin_s[is_bd * 2 + s] = jnp.sin(packed)
        for s in (0, 1):
            rows = slice(s * LANES, (s + 1) * LANES)
            cos_b[rows], sin_b[rows] = over_pairs(cos_s[is_bd * 2 + s], sin_s[is_bd * 2 + s], hf * 64)
            inv_b[rows] = jnp.broadcast_to(abuf[base + s, pl.ds(LANES + hf, 1)], (LANES, LANES)).T
        y_val = ybuf[pl.ds(base, 2), pl.ds(pl.multiple_of(hf * LANES, LANES), LANES)].reshape(TOK, D)

        def k_dot(hp):
            cols = pl.ds(pl.multiple_of(cc * HALF + hp * WIDE, WIDE), WIDE)
            k_f[:, hp * WIDE:(hp + 1) * WIDE] = dot(y_val, wk[:, cols])

        def k_rope(h):
            cols = pl.ds(pl.multiple_of(cc * HALF + h * LANES, LANES), LANES)
            val = (k_f[:, h * LANES:(h + 1) * LANES] + vec[BK:BK + 1, cols]) * inv_b[...] * vec[GK:GK + 1, cols]
            k_b[:, h * LANES:(h + 1) * LANES] = (val * cos_b[...] + swap_pairs(val) * sin_b[...]).astype(BF16)

        def v_dot(hp):
            cols = pl.ds(pl.multiple_of(cc * HALF + hp * WIDE, WIDE), WIDE)
            wide = slice(hp * WIDE, (hp + 1) * WIDE)
            v_b[:, wide] = (dot(y_val, wv[:, wide]) + vec[BV:BV + 1, cols]).astype(BF16)

        def score(h):
            cols = slice(h * LANES, (h + 1) * LANES)
            sc = dot(k_b[:, cols], q_t[cols])
            sc_s[h % 3] = sc
            m_old = m_s[h]
            m_new = jnp.maximum(m_old, jnp.max(sc, axis=0, keepdims=True) * EXP_SCALE)
            m_s[h] = m_new
            return m_new, jnp.exp2(m_old - m_new)

        def weigh(h, m_new, alpha):
            w = jnp.exp2(sc_s[h % 3] * EXP_SCALE - m_new)
            l_s[h] = l_s[h] * alpha + jnp.sum(w.reshape(32, 8, 2 * TOK), axis=0)
            w_s[h % 2] = w.astype(BF16)

        def add_up(h, alpha):
            cols = slice(h * LANES, (h + 1) * LANES)
            acc[h] = acc[h] * alpha + dot_dims(v_b[:, cols], w_s[h % 2], 0, 0)

        for hp in range(3):
            k_dot(hp)
        for hp in range(3):
            v_dot(hp)
        for h in range(6):
            k_rope(h)
        st = {0: score(0), 1: score(1)}
        for h in range(6):
            weigh(h, *st[h])
            if h + 2 < 6:
                st[h + 2] = score(h + 2)
            add_up(h, st[h][1])
        return 0

    lax.fori_loop(0, 16, body, 0)

    for h in range(6):
        cols = slice(h * LANES, (h + 1) * LANES)
        o_h = (acc[h] / jnp.sum(l_s[h], axis=0, keepdims=True)).T.astype(BF16)
        obuf[0, :, cols] = o_h[:TOK]
        obuf[1, :, cols] = o_h[TOK:]
    send_o = pltpu.make_async_remote_copy(obuf.at[1 - cc], o_hbm.at[cc], qo_s.at[1], qo_r.at[1], device_id=dev[CP], device_id_type=MESH)
    got_o = pltpu.make_async_remote_copy(obuf.at[1 - cc], o_hbm.at[1 - cc], qo_s.at[1], qo_r.at[1], device_id=dev[CP], device_id_type=MESH)
    keep_o = pltpu.make_async_copy(obuf.at[cc], o_hbm.at[cc], loc.at[10])
    send_o.start()
    keep_o.start()

    sent(mine, YP, DU, M1, AX, X2)
    sent(mine, CP, X1, X2, AX)
    sent(peer0, CP, DU)

    def sent_z(to):
        sent(mine, to, X1, AX, X2)
        sent(peer0, to, DU)
    along_z(sent_z)
    for i in (1, 2, 3):
        slot = slot_a(i)
        peer = slot_b(i)

        def sent_on(to, slot=slot, peer=peer):
            sent(slot, to, X1, AX, X2)
            sent(peer, to, DU)
        relay(i, sent_on)
        sent(slot, YP, M1, AX, X2)
        sent(slot, CP, X1, AX, X2)
        sent(peer, CP, DU)
    for i in range(4):
        sent(slot_b(i), CP, M1, AX, X2)
    send_q.wait_send()
    pltpu.make_async_copy(ck, ck_hbm, loc.at[8]).wait()
    pltpu.make_async_copy(cvt, cvt_hbm, loc.at[9]).wait()
    send_o.wait_send()
    keep_o.wait()
    got_o.wait_recv()


def gather_attention(*args):
    any_spec = pl.BlockSpec(memory_space=pl.ANY)
    vmem_spec = pl.BlockSpec(memory_space=pltpu.VMEM)
    keys = 16 * TOK
    square = pltpu.VMEM((D, D), BF16)
    return pl.pallas_call(
        attn_kernel,
        out_shape=[jax.ShapeDtypeStruct((2, TOK, HALF), BF16), jax.ShapeDtypeStruct((TEXT, D), BF16), jax.ShapeDtypeStruct((D, TEXT), BF16)],
        in_specs=[any_spec] * 8 + [vmem_spec] * 8,
        out_specs=[any_spec] * 3,
        scratch_shapes=[
            pltpu.VMEM((TOK, D), BF16), pltpu.VMEM((HEAD // 2, TOK), F32), pltpu.VMEM((TEXT, D), BF16),
            square, square, pltpu.VMEM((D, HALF), BF16), square, square, pltpu.VMEM((8, D), F32),
            pltpu.VMEM((16, TOK, D), BF16), pltpu.VMEM((16, AUX, LANES), F32), pltpu.VMEM((TOK, D), F32),
            pltpu.VMEM((2, TOK, HALF), BF16), pltpu.VMEM((TOK, HALF), BF16), pltpu.VMEM((HALF, 2 * TOK), BF16),
            pltpu.VMEM((TOK, HALF), BF16), pltpu.VMEM((TOK, HALF), BF16),
            pltpu.VMEM((4, LANES, LANES), F32), pltpu.VMEM((4, LANES, LANES), F32),
            pltpu.VMEM((TOK, LANES), F32), pltpu.VMEM((TOK, LANES), F32), pltpu.VMEM((TOK, LANES), F32),
            pltpu.VMEM((6, HEAD, 2 * TOK), F32), pltpu.VMEM((6, 1, 2 * TOK), F32), pltpu.VMEM((6, 8, 2 * TOK), F32),
            pltpu.VMEM((TOK, HALF), F32), pltpu.VMEM((3, TOK, 2 * TOK), F32), pltpu.VMEM((2, TOK, 2 * TOK), BF16),
            pltpu.VMEM((TEXT, D), F32), pltpu.VMEM((TEXT, D), BF16), pltpu.VMEM((D, TEXT), BF16), pltpu.VMEM((2, TOK, LANES), F32),
            pltpu.VMEM((2, TOK, HALF), BF16),
            pltpu.SemaphoreType.DMA((4, 16)), pltpu.SemaphoreType.DMA((4, 4, 16)), pltpu.SemaphoreType.DMA((11,)),
            pltpu.SemaphoreType.DMA((2,)), pltpu.SemaphoreType.DMA((2,)),
        ],
        cost_estimate=pl.CostEstimate(flops=2 * keys * D * D + 4 * keys * HALF * 2 * TOK, bytes_accessed=10 * D * D, transcendentals=6 * keys * 2 * TOK),
        compiler_params=pltpu.CompilerParams(collective_id=0, has_side_effects=True, vmem_limit_bytes=VMEM_MAX),
        name="gather_attention",
    )(*args)


def tail_kernel(o_hbm, x_hbm, ck_hbm, cvt_hbm, wo_hbm, cwq_hbm, cwo_hbm, w1_hbm, w2_hbm,
                temb_ref, mod_ref, bo_ref, nw_ref, nb_ref, cgq_ref, out_ref,
                o_v, x_v, ck, cvt, wo, cwq, cwo, w1, w2, vec, res, lin, act, u_b, ssq, sems, ring):
    n_ff = FF // FT

    def ff_copies(t, slot):
        cols = pl.ds(pl.multiple_of(t * FT, FT), FT)
        return (pltpu.make_async_copy(w1_hbm.at[:, cols], w1.at[slot], ring.at[0, slot]),
                pltpu.make_async_copy(w2_hbm.at[cols], w2.at[slot], ring.at[1, slot]))

    gets = [pltpu.make_async_copy(src, dst, sems.at[n]) for n, (src, dst) in enumerate(
        ((o_hbm, o_v), (wo_hbm, wo), (x_hbm.at[0], x_v), (cwq_hbm, cwq), (ck_hbm, ck), (cvt_hbm, cvt), (cwo_hbm, cwo)))]
    get_o, get_wo, get_x, get_cwq, get_ck, get_cvt, get_cwo = gets
    for get in (get_o, get_wo, get_x, get_cwq):
        get.start()
    for row in range(6):
        vec[row:row + 1] = ada_row(temb_ref, mod_ref, row)
    BO, NW, NB, CGQ = 6, 7, 8, 9
    for row, ref in ((BO, bo_ref), (NW, nw_ref), (NB, nb_ref), (CGQ, cgq_ref)):
        vec[row:row + 1] = as_row(ref)

    get_o.wait()
    get_wo.wait()
    for get in (get_ck, get_cvt, get_cwo):
        get.start()
    get_x.wait()

    @pl.loop(0, 6)
    def _(j):
        cols = tile256(j)
        prod = dot(o_v[0], wo[0:HALF, cols]) + dot(o_v[1], wo[HALF:D, cols])
        res[:, cols] = x_v[:, cols].astype(F32) + vec[2:3, cols] * (prod + vec[BO:BO + 1, cols])

    @pl.loop(0, TOK // 32)
    def _(part):
        rows = pl.ds(pl.multiple_of(part * 32, 32), 32)
        act[rows] = (layer_norm_rows(res[rows]) * vec[NW:NW + 1] + vec[NB:NB + 1]).astype(BF16)
    get_cwq.wait()
    for t in range(RING):
        for get in ff_copies(t, t):
            get.start()
    ssq[...] = jnp.zeros_like(ssq)

    @pl.loop(0, 6)
    def _(j):
        prod = dot(act[...], cwq[:, tile256(j)])
        lin[:, tile256(j)] = prod
        ssq[...] += fold_sq(prod)
    q_inv = inv_rms(ssq[...])
    get_ck.wait()
    get_cvt.wait()

    @pl.loop(0, HEADS // 2)
    def _(hp):
        for h2 in (0, 1):
            cols = tile128(hp * 2 + h2)
            q_h = (lin[:, cols] * q_inv * vec[CGQ:CGQ + 1, cols]).astype(BF16)
            sc = dot_dims(ck[:, cols], q_h, 1, 1)
            m_row = jnp.max(sc, axis=0, keepdims=True) * EXP_SCALE
            w = jnp.exp2(sc * EXP_SCALE - m_row)
            o_t = dot(cvt[cols, :], w.astype(BF16)) / jnp.sum(w, axis=0, keepdims=True)
            act[:, cols] = o_t.T.astype(BF16)
    get_cwo.wait()

    @pl.loop(0, 6)
    def _(j):
        cols = tile256(j)
        res[:, cols] += dot(act[...], cwo[:, cols])

    @pl.loop(0, TOK // 32)
    def _(part):
        rows = pl.ds(pl.multiple_of(part * 32, 32), 32)
        act[rows] = (layer_norm_rows(res[rows]) * (1.0 + vec[4:5]) + vec[3:4]).astype(BF16)
        lin[rows] = jnp.zeros((32, D), F32)

    def ffn(t, _):
        slot = t % RING
        for get in ff_copies(t, slot):
            get.wait()
        for s in range(FT // WIDE):
            cols = slice(s * WIDE, (s + 1) * WIDE)
            u_b[:, cols] = jax.nn.gelu(dot(act[...], w1[slot, :, cols]), approximate=True).astype(BF16)
        for j in range(6):
            cols = slice(j * WIDE, (j + 1) * WIDE)
            lin[:, cols] += dot(u_b[...], w2[slot, :, cols])

        @pl.when(t + RING < n_ff)
        def _():
            for get in ff_copies(t + RING, slot):
                get.start()
        return 0

    lax.fori_loop(0, n_ff, ffn, 0)

    @pl.loop(0, TOK // 32)
    def _(part):
        rows = pl.ds(pl.multiple_of(part * 32, 32), 32)
        out_ref[0, rows] = (res[rows] + vec[5:6] * lin[rows]).astype(BF16)


def tail(*args):
    any_spec = pl.BlockSpec(memory_space=pl.ANY)
    vmem_spec = pl.BlockSpec(memory_space=pltpu.VMEM)
    square = pltpu.VMEM((D, D), BF16)
    return pl.pallas_call(
        tail_kernel,
        out_shape=jax.ShapeDtypeStruct((1, TOK, D), BF16),
        in_specs=[any_spec] * 9 + [vmem_spec] * 6,
        out_specs=vmem_spec,
        scratch_shapes=[
            pltpu.VMEM((2, TOK, HALF), BF16), pltpu.VMEM((TOK, D), BF16), pltpu.VMEM((TEXT, D), BF16), pltpu.VMEM((D, TEXT), BF16),
            square, square, square, pltpu.VMEM((RING, D, FT), BF16), pltpu.VMEM((RING, FT, D), BF16), pltpu.VMEM((16, D), F32),
            pltpu.VMEM((TOK, D), F32), pltpu.VMEM((TOK, D), F32), pltpu.VMEM((TOK, D), BF16), pltpu.VMEM((TOK, FT), BF16), pltpu.VMEM((TOK, LANES), F32),
            pltpu.SemaphoreType.DMA((7,)), pltpu.SemaphoreType.DMA((2, RING)),
        ],
        cost_estimate=pl.CostEstimate(flops=4 * TOK * D * FF + 6 * TOK * D * D, bytes_accessed=4 * D * FF + 6 * D * D, transcendentals=TOK * FF),
        compiler_params=pltpu.CompilerParams(vmem_limit_bytes=VMEM_MAX),
        name="tail",
    )(*args)


def solution(mesh):
    tok_spec = P('dp', ('sp', 'uly'), None)
    batch_spec = P('dp', None, None)

    def local_block(tokens, rope_ang, t_emb, block_mod, context, attn_wq, attn_bq, attn_wk, attn_bk, attn_wv, attn_bv, attn_gq, attn_gk, attn_wo, attn_bo, norm3_w, norm3_b, cross_wq, cross_wk, cross_wv, cross_gq, cross_gk, cross_wo, ffn_w1, ffn_w2):
        o_half, cross_k, cross_vt = gather_attention(tokens, rope_ang.T, context, attn_wq, attn_wk, attn_wv, cross_wk, cross_wv, t_emb.reshape(-1), block_mod.reshape(-1), attn_bq, attn_bk, attn_bv, attn_gq, attn_gk, cross_gk)
        return tail(o_half, tokens, cross_k, cross_vt, attn_wo, cross_wq, cross_wo, ffn_w1, ffn_w2, t_emb.reshape(-1), block_mod.reshape(-1), attn_bo, norm3_w, norm3_b, cross_gq)

    in_specs = (tok_spec, P(('sp', 'uly'), None), batch_spec, P(), batch_spec) + (P(),) * 20
    return jax.shard_map(local_block, mesh=mesh, in_specs=in_specs, out_specs=tok_spec, check_vma=False)
```

```python
import math

import jax
import jax.numpy as jnp
from jax import lax
from jax.experimental import pallas as pl
from jax.experimental.pallas import tpu as pltpu
from jax.sharding import PartitionSpec as P

EPS = 1e-6
HEAD = 128
LANES = 128
HEADS = 12
D = 1536
FF = 8960
TOK = 256
WIDE = 256
TEXT = 512
HALF = 768
DUAL = 32
AUX = 136
FT = 1280
RING = 4
MESH = pl.DeviceIdType.MESH
EXP_SCALE = math.log2(math.e) * HEAD ** -0.5
F32 = jnp.float32
BF16 = jnp.bfloat16
VMEM_MAX = 67043328


def dot(lhs, rhs):
    return jnp.dot(lhs, rhs, preferred_element_type=F32)


def dot_dims(lhs, rhs, l_dim, r_dim):
    return lax.dot_general(lhs, rhs, (((l_dim,), (r_dim,)), ((), ())), preferred_element_type=F32)


def swap_pairs(val):
    lane = lax.broadcasted_iota(jnp.int32, val.shape, 1)
    return jnp.where(lane % 2 == 0, pltpu.roll(val, 127, 1), pltpu.roll(val, 1, 1))


def over_pairs(cos_p, sin_p, base):
    lane = lax.broadcasted_iota(jnp.int32, (LANES, LANES), 1)
    sign = jnp.where(lane % 2 == 0, -1.0, 1.0).astype(F32)
    pair = lane // 2 + base
    return jnp.take_along_axis(cos_p, pair, axis=1), jnp.take_along_axis(sin_p, pair, axis=1) * sign


def layer_norm_rows(x_f32):
    centered = x_f32 - jnp.mean(x_f32, axis=-1, keepdims=True)
    var = jnp.mean(centered * centered, axis=-1, keepdims=True)
    return centered * lax.rsqrt(var + EPS)


def fold_sq(val):
    return val[:, :LANES] * val[:, :LANES] + val[:, LANES:] * val[:, LANES:]


def inv_rms(ssq):
    return lax.rsqrt(jnp.sum(ssq, axis=1, keepdims=True) * (1.0 / D) + EPS)


def tile256(j):
    return slice(j * WIDE, (j + 1) * WIDE)


def ada_row(temb_ref, mod_ref, row):
    cols = slice(row * D, (row + 1) * D)
    return (temb_ref[cols] + mod_ref[cols]).reshape(1, D)


def as_row(ref):
    return ref[...].astype(F32).reshape(1, D)


def attn_kernel(x_hbm, ang_hbm, c_hbm, wq_hbm, wk_hbm, wv_hbm, cwk_hbm, cwv_hbm,
                temb_ref, mod_ref, bq_ref, bk_ref, bv_ref, gq_ref, gk_ref, cgk_ref,
                o_hbm, ck_hbm, cvt_hbm,
                xbuf, ang, ctx, wq, wk, wv, cwk, cwv, vec,
                ybuf, abuf, raw, q_loc, q_got, q_t, k_b, v_b, cos_s, sin_s, cos_b, sin_b, inv_b, acc, m_s, l_s, k_f, sc_s, w_s,
                craw, ck, cvt, ssq, obuf,
                rs, ss, loc, qo_s, qo_r):
    z = lax.axis_index('sp')
    u = lax.axis_index('uly')
    yy = u // 2
    cc = u % 2
    hi = z // 2
    zm = z * (1 - hi) + (3 - z) * hi
    UP, DN, YP, CP = 0, 1, 2, 3
    dev = ({'sp': (z + 1) % 4, 'uly': u}, {'sp': (z + 3) % 4, 'uly': u},
           {'sp': z, 'uly': (1 - yy) * 2 + cc}, {'sp': z, 'uly': yy * 2 + 1 - cc})
    ends = jnp.logical_or(z == 0, z == 3)
    mids = jnp.logical_and(z > 0, z < 3)

    def z_of(i):
        low = i // 2
        m_i = low * i + (1 - low) * (i + zm - 2 * i * zm)
        return m_i * (1 - hi) + (3 - m_i) * hi

    def slot_a(i):
        return z_of(i) * 4 + yy * 2 + cc

    def slot_b(i):
        return z_of(i) * 4 + (1 - yy) * 2 + cc

    def slot_c(i):
        return z_of(i) * 4 + yy * 2 + 1 - cc

    def slot_d(i):
        return z_of(i) * 4 + (1 - yy) * 2 + 1 - cc

    X1, X2, DU, M1, AX = 'x1', 'x2', 'du', 'm1', 'ax'
    rows_of = {X1: (0, LANES), X2: (LANES, LANES), DU: (0, DUAL), M1: (DUAL, LANES - DUAL)}
    sem_of = {X1: 0, M1: 0, X2: 1, DU: 2, AX: 3}

    def copy(slot, part, to):
        ref = abuf.at[slot] if part == AX else ybuf.at[slot, pl.ds(*rows_of[part])]
        key = sem_of[part]
        return pltpu.make_async_remote_copy(ref, ref, ss.at[to, key, slot], rs.at[key, slot], device_id=dev[to], device_id_type=MESH)

    def start(slot, to, *parts):
        for part in parts:
            copy(slot, part, to).start()

    def got(slot, *parts):
        for part in parts:
            copy(slot, part, CP).wait_recv()

    def sent(slot, to, *parts):
        for part in parts:
            copy(slot, part, to).wait_send()

    def along_z(act):
        @pl.when(z < 3)
        def _():
            act(UP)

        @pl.when(z > 0)
        def _():
            act(DN)

    def relay(i, act):
        to_1 = (UP, DN, DN)[i - 1]
        to_2 = (DN, UP, UP)[i - 1]

        @pl.when(z == 1)
        def _():
            act(to_1)

        @pl.when(z == 2)
        def _():
            act(to_2)

    barrier = pltpu.get_barrier_semaphore()
    for to in (YP, CP):
        pl.semaphore_signal(barrier, 1, device_id=dev[to], device_id_type=MESH)
    along_z(lambda to: pl.semaphore_signal(barrier, 1, device_id=dev[to], device_id_type=MESH))

    get_x = pltpu.make_async_copy(x_hbm.at[0], xbuf, loc.at[0])
    get_ang = pltpu.make_async_copy(ang_hbm, ang, loc.at[1])
    get_wk = pltpu.make_async_copy(wk_hbm, wk, loc.at[2])
    get_wq = pltpu.make_async_copy(wq_hbm, wq, loc.at[3])
    get_wv = pltpu.make_async_copy(wv_hbm.at[:, pl.ds(pl.multiple_of(cc * HALF, HALF), HALF)], wv, loc.at[4])
    get_ctx = pltpu.make_async_copy(c_hbm.at[0], ctx, loc.at[5])
    get_cwk = pltpu.make_async_copy(cwk_hbm, cwk, loc.at[6])
    get_cwv = pltpu.make_async_copy(cwv_hbm, cwv, loc.at[7])
    for get in (get_x, get_ang, get_wk):
        get.start()
    BQ, BK, BV, GQ, GK, CGK = range(6)
    for row, ref in enumerate((bq_ref, bk_ref, bv_ref, gq_ref, gk_ref, cgk_ref)):
        vec[row:row + 1] = as_row(ref)
    shift = ada_row(temb_ref, mod_ref, 0)
    scale = 1.0 + ada_row(temb_ref, mod_ref, 1)
    mine = slot_a(0)
    get_x.wait()
    get_wq.start()

    for part in range(TOK // 32):
        rows = slice(part * 32, (part + 1) * 32)
        ybuf[mine, rows] = (layer_norm_rows(xbuf[rows].astype(F32)) * scale + shift).astype(BF16)

    @pl.when(ends)
    def _():
        pl.semaphore_wait(barrier, 3)

    @pl.when(mids)
    def _():
        pl.semaphore_wait(barrier, 4)

    start(mine, YP, DU, M1)
    along_z(lambda to: start(mine, to, X1))
    start(mine, CP, X1, X2)

    get_ang.wait()
    abuf[mine, 0:LANES] = jnp.concatenate([ang[:, 0:LANES], ang[:, LANES:WIDE]], axis=0).T
    ssq[0] = jnp.zeros((TOK, LANES), F32)
    ssq[1] = jnp.zeros((TOK, LANES), F32)
    get_wk.wait()
    for get in (get_wv, get_ctx, get_cwk, get_cwv):
        get.start()

    for j in range(6):
        ssq[0] += fold_sq(dot(ybuf[mine], wk[:, tile256(j)]) + vec[BK:BK + 1, tile256(j)])
    k_inv = inv_rms(ssq[0])
    for part in (0, 1):
        abuf[mine, LANES + part:129 + part] = jnp.broadcast_to(k_inv[part * LANES:(part + 1) * LANES], (LANES, LANES)).T[0:1]
    abuf[mine, 130:136] = jnp.zeros((6, LANES), F32)
    start(mine, YP, AX, X2)
    along_z(lambda to: start(mine, to, AX, X2))
    start(mine, CP, AX)

    get_wq.wait()

    for j in range(6):
        lin = dot(ybuf[mine], wq[:, tile256(j)]) + vec[BQ:BQ + 1, tile256(j)]
        raw[:, tile256(j)] = lin
        ssq[1] += fold_sq(lin)
    q_inv = inv_rms(ssq[1])
    packed = abuf[mine, 0:LANES]
    cos_p = jnp.cos(packed)
    sin_p = jnp.sin(packed)
    for part in (0, 1):
        rows = pl.ds(part * LANES, LANES)
        cos_d, sin_d = over_pairs(cos_p, sin_p, part * 64)
        for h in range(HEADS):
            cols = slice(h * LANES, (h + 1) * LANES)
            val = raw[rows, cols] * q_inv[part * LANES:(part + 1) * LANES] * vec[GQ:GQ + 1, cols]
            q_loc[h // 6, rows, (h % 6) * LANES:(h % 6 + 1) * LANES] = (val * cos_d + swap_pairs(val) * sin_d).astype(BF16)
    send_q = pltpu.make_async_remote_copy(q_loc.at[1 - cc], q_got, qo_s.at[0], qo_r.at[0], device_id=dev[CP], device_id_type=MESH)
    send_q.start()

    peer0 = slot_b(0)
    got(peer0, DU)
    along_z(lambda to: start(peer0, to, DU))
    start(peer0, CP, DU)

    def event_a(i, hf):
        slot = slot_a(i)
        peer = slot_b(i)
        if hf:
            got(slot, X2)
            relay(i, lambda to: start(slot, to, X2))
            start(slot, YP, X2)
            start(slot, CP, X2)
        else:
            got(slot, X1, AX)
            relay(i, lambda to: start(slot, to, X1, AX))
            start(slot, YP, M1, AX)
            start(slot, CP, X1, AX)
            got(peer, DU)
            relay(i, lambda to: start(peer, to, DU))
            start(peer, CP, DU)

    def event_b(i, hf):
        slot = slot_b(i)
        parts = (X2,) if hf else (M1, AX)
        got(slot, *parts)
        start(slot, CP, *parts)

    for h in range(6):
        cols = slice(h * LANES, (h + 1) * LANES)
        q_t[cols, pl.ds(pl.multiple_of(cc * TOK, TOK), TOK)] = q_loc[cc, :, cols].T
    acc[...] = jnp.zeros_like(acc)
    l_s[...] = jnp.zeros_like(l_s)
    m_s[...] = jnp.full_like(m_s, -jnp.inf)
    send_q.wait_recv()
    for h in range(6):
        cols = slice(h * LANES, (h + 1) * LANES)
        q_t[cols, pl.ds(pl.multiple_of((1 - cc) * TOK, TOK), TOK)] = q_got[:, cols].T
    get_wv.wait()

    def cross_k():
        get_ctx.wait()
        get_cwk.wait()
        ssq[...] = jnp.zeros_like(ssq)

        for j in range(6):
            lin = dot(ctx[...], cwk[:, tile256(j)])
            craw[:, tile256(j)] = lin
            sq = fold_sq(lin)
            ssq[0] += sq[:TOK]
            ssq[1] += sq[TOK:]
        inv_0 = inv_rms(ssq[0])
        inv_1 = inv_rms(ssq[1])

        for j in range(6):
            gain = vec[CGK:CGK + 1, tile256(j)]
            ck[0:TOK, tile256(j)] = (craw[0:TOK, tile256(j)] * inv_0 * gain).astype(BF16)
            ck[TOK:TEXT, tile256(j)] = (craw[TOK:TEXT, tile256(j)] * inv_1 * gain).astype(BF16)
        pltpu.make_async_copy(ck, ck_hbm, loc.at[8]).start()

    def cross_v():
        get_cwv.wait()

        for j in range(6):
            cvt[tile256(j), :] = dot(ctx[...], cwv[:, tile256(j)]).astype(BF16).T
        pltpu.make_async_copy(cvt, cvt_hbm, loc.at[9]).start()

    at_ends = {2: ('a', 1, 0), 4: ('a', 1, 1), 6: ('a', 2, 0), 8: ('a', 2, 1), 10: ('a', 3, 0), 12: ('a', 3, 1)}
    at_mids = {2: ('a', 1, 0, 2, 0), 4: ('a', 1, 1, 2, 1), 8: ('a', 3, 0), 10: ('a', 3, 1)}
    at_all = {3: (0, 0), 5: (0, 1), 7: (1, 0), 9: (1, 1), 11: (2, 0), 13: (2, 1), 14: (3, 0), 15: (3, 1)}

    def body(it, _):
        first = (15 - it) // 14
        last = it // 14
        mid = 1 - first - last
        r = (it + 2) % 4
        k = (it + 2) // 4 - 1
        is_bd = mid * (r % 2) + last
        hf = mid * (r // 2) + (first + last) * (it % 2)
        idx = mid * (k + 1 - r % 2) + last * 3

        for step in range(16):
            has_ends, has_mids, has_all = step in at_ends, step in at_mids, step in at_all
            if not (has_ends or has_mids or has_all):
                continue

            @pl.when(it == step)
            def _(step=step, has_ends=has_ends, has_mids=has_mids, has_all=has_all):
                if has_ends:
                    @pl.when(ends)
                    def _():
                        event_a(*at_ends[step][1:3])
                if has_mids:
                    @pl.when(mids)
                    def _():
                        todo = at_mids[step][1:]
                        for n in range(0, len(todo), 2):
                            event_a(todo[n], todo[n + 1])
                if has_all:
                    event_b(*at_all[step])

        pl.when(it == 4)(cross_k)
        pl.when(it == 8)(cross_v)

        @pl.when(jnp.logical_and(is_bd == 0, hf == 0))
        def _():
            got(slot_c(idx), X1, AX)

        @pl.when(jnp.logical_and(is_bd == 0, hf == 1))
        def _():
            got(slot_c(idx), X2)

        @pl.when(jnp.logical_and(is_bd == 1, hf == 0))
        def _():
            got(slot_d(idx), DU, M1, AX)

        @pl.when(jnp.logical_and(is_bd == 1, hf == 1))
        def _():
            got(slot_d(idx), X2)

        y_of = (1 - is_bd) * yy + is_bd * (1 - yy)
        base = z_of(idx) * 4 + y_of * 2

        @pl.when(hf == 0)
        def _():
            for s in (0, 1):
                packed = abuf[base + s, 0:LANES]
                cos_s[is_bd * 2 + s] = jnp.cos(packed)
                sin_s[is_bd * 2 + s] = jnp.sin(packed)
        for s in (0, 1):
            rows = slice(s * LANES, (s + 1) * LANES)
            cos_b[rows], sin_b[rows] = over_pairs(cos_s[is_bd * 2 + s], sin_s[is_bd * 2 + s], hf * 64)
            inv_b[rows] = jnp.broadcast_to(abuf[base + s, pl.ds(LANES + hf, 1)], (LANES, LANES)).T
        y_val = ybuf[pl.ds(base, 2), pl.ds(pl.multiple_of(hf * LANES, LANES), LANES)].reshape(TOK, D)

        def k_dot(hp):
            cols = pl.ds(pl.multiple_of(cc * HALF + hp * WIDE, WIDE), WIDE)
            k_f[:, hp * WIDE:(hp + 1) * WIDE] = dot(y_val, wk[:, cols])

        def k_rope(h):
            cols = pl.ds(pl.multiple_of(cc * HALF + h * LANES, LANES), LANES)
            val = (k_f[:, h * LANES:(h + 1) * LANES] + vec[BK:BK + 1, cols]) * inv_b[...] * vec[GK:GK + 1, cols]
            k_b[:, h * LANES:(h + 1) * LANES] = (val * cos_b[...] + swap_pairs(val) * sin_b[...]).astype(BF16)

        def v_dot(hp):
            cols = pl.ds(pl.multiple_of(cc * HALF + hp * WIDE, WIDE), WIDE)
            wide = slice(hp * WIDE, (hp + 1) * WIDE)
            v_b[:, wide] = (dot(y_val, wv[:, wide]) + vec[BV:BV + 1, cols]).astype(BF16)

        def score(h):
            cols = slice(h * LANES, (h + 1) * LANES)
            sc = dot(k_b[:, cols], q_t[cols])
            sc_s[h % 3] = sc
            m_old = m_s[h]
            m_new = jnp.maximum(m_old, jnp.max(sc, axis=0, keepdims=True) * EXP_SCALE)
            m_s[h] = m_new
            return m_new, jnp.exp2(m_old - m_new)

        def weigh(h, m_new, alpha):
            w = jnp.exp2(sc_s[h % 3] * EXP_SCALE - m_new)
            l_s[h] = l_s[h] * alpha + jnp.sum(w.reshape(32, 8, 2 * TOK), axis=0)
            w_s[h % 2] = w.astype(BF16)

        def add_up(h, alpha):
            cols = slice(h * LANES, (h + 1) * LANES)
            acc[h] = acc[h] * alpha + dot_dims(v_b[:, cols], w_s[h % 2], 0, 0)

        for hp in range(3):
            k_dot(hp)
        for hp in range(3):
            v_dot(hp)
        for h in range(6):
            k_rope(h)
        st = {0: score(0), 1: score(1)}
        for h in range(6):
            weigh(h, *st[h])
            if h + 2 < 6:
                st[h + 2] = score(h + 2)
            add_up(h, st[h][1])
        return 0

    lax.fori_loop(0, 16, body, 0)

    for h in range(6):
        cols = slice(h * LANES, (h + 1) * LANES)
        o_h = (acc[h] / jnp.sum(l_s[h], axis=0, keepdims=True)).T.astype(BF16)
        obuf[0, :, cols] = o_h[:TOK]
        obuf[1, :, cols] = o_h[TOK:]
    send_o = pltpu.make_async_remote_copy(obuf.at[1 - cc], o_hbm.at[cc], qo_s.at[1], qo_r.at[1], device_id=dev[CP], device_id_type=MESH)
    got_o = pltpu.make_async_remote_copy(obuf.at[1 - cc], o_hbm.at[1 - cc], qo_s.at[1], qo_r.at[1], device_id=dev[CP], device_id_type=MESH)
    keep_o = pltpu.make_async_copy(obuf.at[cc], o_hbm.at[cc], loc.at[10])
    send_o.start()
    keep_o.start()

    sent(mine, YP, DU, M1, AX, X2)
    sent(mine, CP, X1, X2, AX)
    sent(peer0, CP, DU)

    def sent_z(to):
        sent(mine, to, X1, AX, X2)
        sent(peer0, to, DU)
    along_z(sent_z)
    for i in (1, 2, 3):
        slot = slot_a(i)
        peer = slot_b(i)

        def sent_on(to, slot=slot, peer=peer):
            sent(slot, to, X1, AX, X2)
            sent(peer, to, DU)
        relay(i, sent_on)
        sent(slot, YP, M1, AX, X2)
        sent(slot, CP, X1, AX, X2)
        sent(peer, CP, DU)
    for i in range(4):
        sent(slot_b(i), CP, M1, AX, X2)
    send_q.wait_send()
    pltpu.make_async_copy(ck, ck_hbm, loc.at[8]).wait()
    pltpu.make_async_copy(cvt, cvt_hbm, loc.at[9]).wait()
    send_o.wait_send()
    keep_o.wait()
    got_o.wait_recv()


def gather_attention(*args):
    any_spec = pl.BlockSpec(memory_space=pl.ANY)
    vmem_spec = pl.BlockSpec(memory_space=pltpu.VMEM)
    keys = 16 * TOK
    square = pltpu.VMEM((D, D), BF16)
    return pl.pallas_call(
        attn_kernel,
        out_shape=[jax.ShapeDtypeStruct((2, TOK, HALF), BF16), jax.ShapeDtypeStruct((TEXT, D), BF16), jax.ShapeDtypeStruct((D, TEXT), BF16)],
        in_specs=[any_spec] * 8 + [vmem_spec] * 8,
        out_specs=[any_spec] * 3,
        scratch_shapes=[
            pltpu.VMEM((TOK, D), BF16), pltpu.VMEM((HEAD // 2, TOK), F32), pltpu.VMEM((TEXT, D), BF16),
            square, square, pltpu.VMEM((D, HALF), BF16), square, square, pltpu.VMEM((8, D), F32),
            pltpu.VMEM((16, TOK, D), BF16), pltpu.VMEM((16, AUX, LANES), F32), pltpu.VMEM((TOK, D), F32),
            pltpu.VMEM((2, TOK, HALF), BF16), pltpu.VMEM((TOK, HALF), BF16), pltpu.VMEM((HALF, 2 * TOK), BF16),
            pltpu.VMEM((TOK, HALF), BF16), pltpu.VMEM((TOK, HALF), BF16),
            pltpu.VMEM((4, LANES, LANES), F32), pltpu.VMEM((4, LANES, LANES), F32),
            pltpu.VMEM((TOK, LANES), F32), pltpu.VMEM((TOK, LANES), F32), pltpu.VMEM((TOK, LANES), F32),
            pltpu.VMEM((6, HEAD, 2 * TOK), F32), pltpu.VMEM((6, 1, 2 * TOK), F32), pltpu.VMEM((6, 8, 2 * TOK), F32),
            pltpu.VMEM((TOK, HALF), F32), pltpu.VMEM((3, TOK, 2 * TOK), F32), pltpu.VMEM((2, TOK, 2 * TOK), BF16),
            pltpu.VMEM((TEXT, D), F32), pltpu.VMEM((TEXT, D), BF16), pltpu.VMEM((D, TEXT), BF16), pltpu.VMEM((2, TOK, LANES), F32),
            pltpu.VMEM((2, TOK, HALF), BF16),
            pltpu.SemaphoreType.DMA((4, 16)), pltpu.SemaphoreType.DMA((4, 4, 16)), pltpu.SemaphoreType.DMA((11,)),
            pltpu.SemaphoreType.DMA((2,)), pltpu.SemaphoreType.DMA((2,)),
        ],
        cost_estimate=pl.CostEstimate(flops=2 * keys * D * D + 4 * keys * HALF * 2 * TOK, bytes_accessed=10 * D * D, transcendentals=6 * keys * 2 * TOK),
        compiler_params=pltpu.CompilerParams(collective_id=0, has_side_effects=True, vmem_limit_bytes=VMEM_MAX),
        name="gather_attention",
    )(*args)


def tail_kernel(o_hbm, x_hbm, ck_hbm, cvt_hbm, wo_hbm, cwq_hbm, cwo_hbm, w1_hbm, w2_hbm,
                temb_ref, mod_ref, bo_ref, nw_ref, nb_ref, cgq_ref, out_ref,
                o_v, x_v, ck, cvt, wo, cwq, cwo, w1, w2, vec, res, lin, act, u_b, ssq, sc_s, w_s, sems, ring):
    n_ff = FF // FT

    def ff_copies(t, slot):
        cols = pl.ds(pl.multiple_of(t * FT, FT), FT)
        return (pltpu.make_async_copy(w1_hbm.at[:, cols], w1.at[slot], ring.at[0, slot]),
                pltpu.make_async_copy(w2_hbm.at[cols], w2.at[slot], ring.at[1, slot]))

    gets = [pltpu.make_async_copy(src, dst, sems.at[n]) for n, (src, dst) in enumerate(
        ((o_hbm, o_v), (wo_hbm, wo), (x_hbm.at[0], x_v), (cwq_hbm, cwq), (ck_hbm, ck), (cvt_hbm, cvt), (cwo_hbm, cwo)))]
    get_o, get_wo, get_x, get_cwq, get_ck, get_cvt, get_cwo = gets
    for get in (get_o, get_wo, get_x, get_cwq):
        get.start()
    for row in range(6):
        vec[row:row + 1] = ada_row(temb_ref, mod_ref, row)
    BO, NW, NB, CGQ = 6, 7, 8, 9
    for row, ref in ((BO, bo_ref), (NW, nw_ref), (NB, nb_ref), (CGQ, cgq_ref)):
        vec[row:row + 1] = as_row(ref)

    get_o.wait()
    get_wo.wait()
    for get in (get_ck, get_cvt, get_cwo):
        get.start()
    get_x.wait()

    for j in range(6):
        cols = tile256(j)
        prod = dot(o_v[0], wo[0:HALF, cols]) + dot(o_v[1], wo[HALF:D, cols])
        res[:, cols] = x_v[:, cols].astype(F32) + vec[2:3, cols] * (prod + vec[BO:BO + 1, cols])

    for part in range(TOK // 32):
        rows = slice(part * 32, (part + 1) * 32)
        act[rows] = (layer_norm_rows(res[rows]) * vec[NW:NW + 1] + vec[NB:NB + 1]).astype(BF16)
    get_cwq.wait()
    for t in range(RING):
        for get in ff_copies(t, t):
            get.start()
    ssq[...] = jnp.zeros_like(ssq)

    for j in range(6):
        prod = dot(act[...], cwq[:, tile256(j)])
        lin[:, tile256(j)] = prod
        ssq[...] += fold_sq(prod)
    q_inv = inv_rms(ssq[...])
    get_ck.wait()
    get_cvt.wait()

    def score(h):
        cols = slice(h * LANES, (h + 1) * LANES)
        q_h = (lin[:, cols] * q_inv * vec[CGQ:CGQ + 1, cols]).astype(BF16)
        sc = dot_dims(ck[:, cols], q_h, 1, 1)
        sc_s[h % 3] = sc
        return jnp.max(sc, axis=0, keepdims=True) * EXP_SCALE

    def weigh(h, m_row):
        w = jnp.exp2(sc_s[h % 3] * EXP_SCALE - m_row)
        w_s[h % 2] = w.astype(BF16)
        return jnp.sum(w, axis=0, keepdims=True)

    def finish(h, total):
        cols = slice(h * LANES, (h + 1) * LANES)
        act[:, cols] = (dot(cvt[cols, :], w_s[h % 2]) / total).T.astype(BF16)

    m_rows = {0: score(0), 1: score(1)}
    total = None
    for h in range(HEADS):
        total_prev, total = total, weigh(h, m_rows[h])
        if h + 2 < HEADS:
            m_rows[h + 2] = score(h + 2)
        if h:
            finish(h - 1, total_prev)
    finish(HEADS - 1, total)
    get_cwo.wait()

    for j in range(6):
        cols = tile256(j)
        res[:, cols] += dot(act[...], cwo[:, cols])

    for part in range(TOK // 32):
        rows = slice(part * 32, (part + 1) * 32)
        act[rows] = (layer_norm_rows(res[rows]) * (1.0 + vec[4:5]) + vec[3:4]).astype(BF16)
        lin[rows] = jnp.zeros((32, D), F32)

    def ffn(t, _):
        slot = t % RING
        for get in ff_copies(t, slot):
            get.wait()
        for s in range(FT // WIDE):
            cols = slice(s * WIDE, (s + 1) * WIDE)
            u_b[:, cols] = jax.nn.gelu(dot(act[...], w1[slot, :, cols]), approximate=True).astype(BF16)
        for j in range(6):
            cols = slice(j * WIDE, (j + 1) * WIDE)
            lin[:, cols] += dot(u_b[...], w2[slot, :, cols])

        @pl.when(t + RING < n_ff)
        def _():
            for get in ff_copies(t + RING, slot):
                get.start()
        return 0

    lax.fori_loop(0, n_ff, ffn, 0)

    for part in range(TOK // 32):
        rows = slice(part * 32, (part + 1) * 32)
        out_ref[0, rows] = (res[rows] + vec[5:6] * lin[rows]).astype(BF16)


def tail(*args):
    any_spec = pl.BlockSpec(memory_space=pl.ANY)
    vmem_spec = pl.BlockSpec(memory_space=pltpu.VMEM)
    square = pltpu.VMEM((D, D), BF16)
    return pl.pallas_call(
        tail_kernel,
        out_shape=jax.ShapeDtypeStruct((1, TOK, D), BF16),
        in_specs=[any_spec] * 9 + [vmem_spec] * 6,
        out_specs=vmem_spec,
        scratch_shapes=[
            pltpu.VMEM((2, TOK, HALF), BF16), pltpu.VMEM((TOK, D), BF16), pltpu.VMEM((TEXT, D), BF16), pltpu.VMEM((D, TEXT), BF16),
            square, square, square, pltpu.VMEM((RING, D, FT), BF16), pltpu.VMEM((RING, FT, D), BF16), pltpu.VMEM((16, D), F32),
            pltpu.VMEM((TOK, D), F32), pltpu.VMEM((TOK, D), F32), pltpu.VMEM((TOK, D), BF16), pltpu.VMEM((TOK, FT), BF16), pltpu.VMEM((TOK, LANES), F32),
            pltpu.VMEM((3, TEXT, TOK), F32), pltpu.VMEM((2, TEXT, TOK), BF16),
            pltpu.SemaphoreType.DMA((7,)), pltpu.SemaphoreType.DMA((2, RING)),
        ],
        cost_estimate=pl.CostEstimate(flops=4 * TOK * D * FF + 6 * TOK * D * D, bytes_accessed=4 * D * FF + 6 * D * D, transcendentals=TOK * FF),
        compiler_params=pltpu.CompilerParams(vmem_limit_bytes=VMEM_MAX),
        name="tail",
    )(*args)


def solution(mesh):
    tok_spec = P('dp', ('sp', 'uly'), None)
    batch_spec = P('dp', None, None)

    def local_block(tokens, rope_ang, t_emb, block_mod, context, attn_wq, attn_bq, attn_wk, attn_bk, attn_wv, attn_bv, attn_gq, attn_gk, attn_wo, attn_bo, norm3_w, norm3_b, cross_wq, cross_wk, cross_wv, cross_gq, cross_gk, cross_wo, ffn_w1, ffn_w2):
        o_half, cross_k, cross_vt = gather_attention(tokens, rope_ang.T, context, attn_wq, attn_wk, attn_wv, cross_wk, cross_wv, t_emb.reshape(-1), block_mod.reshape(-1), attn_bq, attn_bk, attn_bv, attn_gq, attn_gk, cross_gk)
        return tail(o_half, tokens, cross_k, cross_vt, attn_wo, cross_wq, cross_wo, ffn_w1, ffn_w2, t_emb.reshape(-1), block_mod.reshape(-1), attn_bo, norm3_w, norm3_b, cross_gq)

    in_specs = (tok_spec, P(('sp', 'uly'), None), batch_spec, P(), batch_spec) + (P(),) * 20
    return jax.shard_map(local_block, mesh=mesh, in_specs=in_specs, out_specs=tok_spec, check_vma=False)
```

```python
import math

import jax
import jax.numpy as jnp
from jax import lax
from jax.experimental import pallas as pl
from jax.experimental.pallas import tpu as pltpu
from jax.sharding import PartitionSpec as P

EPS = 1e-6
HEAD = 128
LANES = 128
HEADS = 12
D = 1536
FF = 8960
TOK = 256
WIDE = 256
TEXT = 512
HALF = 768
AUX = 136
FT = 1280
RING = 4
MESH = pl.DeviceIdType.MESH
EXP_SCALE = math.log2(math.e) * HEAD ** -0.5
F32 = jnp.float32
BF16 = jnp.bfloat16
VMEM_MAX = 67043328


def dot(lhs, rhs):
    return jnp.dot(lhs, rhs, preferred_element_type=F32)


def dot_dims(lhs, rhs, l_dim, r_dim):
    return lax.dot_general(lhs, rhs, (((l_dim,), (r_dim,)), ((), ())), preferred_element_type=F32)


def swap_pairs(val):
    lane = lax.broadcasted_iota(jnp.int32, val.shape, 1)
    return jnp.where(lane % 2 == 0, pltpu.roll(val, 127, 1), pltpu.roll(val, 1, 1))


def over_pairs(cos_p, sin_p, base):
    lane = lax.broadcasted_iota(jnp.int32, (LANES, LANES), 1)
    sign = jnp.where(lane % 2 == 0, -1.0, 1.0).astype(F32)
    pair = lane // 2 + base
    return jnp.take_along_axis(cos_p, pair, axis=1), jnp.take_along_axis(sin_p, pair, axis=1) * sign


def layer_norm_rows(x_f32):
    centered = x_f32 - jnp.mean(x_f32, axis=-1, keepdims=True)
    var = jnp.mean(centered * centered, axis=-1, keepdims=True)
    return centered * lax.rsqrt(var + EPS)


def fold_sq(val):
    return val[:, :LANES] * val[:, :LANES] + val[:, LANES:] * val[:, LANES:]


def inv_rms(ssq):
    return lax.rsqrt(jnp.sum(ssq, axis=1, keepdims=True) * (1.0 / D) + EPS)


def tile256(j):
    return slice(j * WIDE, (j + 1) * WIDE)


def ada_row(temb_ref, mod_ref, row):
    cols = slice(row * D, (row + 1) * D)
    return (temb_ref[cols] + mod_ref[cols]).reshape(1, D)


def as_row(ref):
    return ref[...].astype(F32).reshape(1, D)


def attn_kernel(x_hbm, ang_hbm, c_hbm, wq_hbm, wk_hbm, wv_hbm, cwk_hbm, cwv_hbm,
                temb_ref, mod_ref, bq_ref, bk_ref, bv_ref, gq_ref, gk_ref, cgk_ref,
                o_hbm, ck_hbm, cvt_hbm,
                xbuf, ang, ctx, wq, wk, wv, cwk, cwv, vec,
                ybuf, abuf, raw, q_loc, q_got, q_t, k_b, v_b, cos_s, sin_s, cos_b, sin_b, inv_b, acc, m_s, l_s, k_f, sc_s, w_s,
                craw, ck, cvt, ssq, obuf,
                rs, ss, loc, qo_s, qo_r):
    z = lax.axis_index('sp')
    u = lax.axis_index('uly')
    yy = u // 2
    cc = u % 2
    hi = z // 2
    zm = z * (1 - hi) + (3 - z) * hi
    UP, DN, YP, CP = 0, 1, 2, 3
    dev = ({'sp': (z + 1) % 4, 'uly': u}, {'sp': (z + 3) % 4, 'uly': u},
           {'sp': z, 'uly': (1 - yy) * 2 + cc}, {'sp': z, 'uly': yy * 2 + 1 - cc})
    ends = jnp.logical_or(z == 0, z == 3)
    mids = jnp.logical_and(z > 0, z < 3)

    def z_of(i):
        low = i // 2
        m_i = low * i + (1 - low) * (i + zm - 2 * i * zm)
        return m_i * (1 - hi) + (3 - m_i) * hi

    def slot_a(i):
        return z_of(i) * 4 + yy * 2 + cc

    def slot_b(i):
        return z_of(i) * 4 + (1 - yy) * 2 + cc

    def slot_c(i):
        return z_of(i) * 4 + yy * 2 + 1 - cc

    def slot_d(i):
        return z_of(i) * 4 + (1 - yy) * 2 + 1 - cc

    X1, X2, AX = range(3)

    def copy(slot, part, to):
        ref = abuf.at[slot] if part == AX else ybuf.at[slot, pl.ds(part * LANES, LANES)]
        return pltpu.make_async_remote_copy(ref, ref, ss.at[to, part, slot], rs.at[part, slot], device_id=dev[to], device_id_type=MESH)

    def start(slot, to, *parts):
        for part in parts:
            copy(slot, part, to).start()

    def got(slot, *parts):
        for part in parts:
            copy(slot, part, CP).wait_recv()

    def sent(slot, to, *parts):
        for part in parts:
            copy(slot, part, to).wait_send()

    def along_z(act):
        @pl.when(z < 3)
        def _():
            act(UP)

        @pl.when(z > 0)
        def _():
            act(DN)

    def leave_ends(act):
        @pl.when(z == 0)
        def _():
            act(UP)

        @pl.when(z == 3)
        def _():
            act(DN)

    def relay(i, act):
        to_1 = (UP, DN, DN)[i - 1]
        to_2 = (DN, UP, UP)[i - 1]

        @pl.when(z == 1)
        def _():
            act(to_1)

        @pl.when(z == 2)
        def _():
            act(to_2)

    barrier = pltpu.get_barrier_semaphore()
    for to in (YP, CP):
        pl.semaphore_signal(barrier, 1, device_id=dev[to], device_id_type=MESH)
    along_z(lambda to: pl.semaphore_signal(barrier, 1, device_id=dev[to], device_id_type=MESH))

    get_x = pltpu.make_async_copy(x_hbm.at[0], xbuf, loc.at[0])
    get_ang = pltpu.make_async_copy(ang_hbm, ang, loc.at[1])
    get_wk = pltpu.make_async_copy(wk_hbm, wk, loc.at[2])
    get_wq = pltpu.make_async_copy(wq_hbm, wq, loc.at[3])
    get_wv = pltpu.make_async_copy(wv_hbm.at[:, pl.ds(pl.multiple_of(cc * HALF, HALF), HALF)], wv, loc.at[4])
    get_ctx = pltpu.make_async_copy(c_hbm.at[0], ctx, loc.at[5])
    get_cwk = pltpu.make_async_copy(cwk_hbm, cwk, loc.at[6])
    get_cwv = pltpu.make_async_copy(cwv_hbm, cwv, loc.at[7])
    for get in (get_x, get_ang, get_wk):
        get.start()
    BQ, BK, BV, GQ, GK, CGK = range(6)
    for row, ref in enumerate((bq_ref, bk_ref, bv_ref, gq_ref, gk_ref, cgk_ref)):
        vec[row:row + 1] = as_row(ref)
    shift = ada_row(temb_ref, mod_ref, 0)
    scale = 1.0 + ada_row(temb_ref, mod_ref, 1)
    mine = slot_a(0)
    get_x.wait()
    get_wq.start()

    for part in range(TOK // 32):
        rows = slice(part * 32, (part + 1) * 32)
        ybuf[mine, rows] = (layer_norm_rows(xbuf[rows].astype(F32)) * scale + shift).astype(BF16)

    @pl.when(ends)
    def _():
        pl.semaphore_wait(barrier, 3)

    @pl.when(mids)
    def _():
        pl.semaphore_wait(barrier, 4)

    start(mine, YP, X1)
    along_z(lambda to: start(mine, to, X1))
    start(mine, CP, X1, X2)

    get_ang.wait()
    abuf[mine, 0:LANES] = jnp.concatenate([ang[:, 0:LANES], ang[:, LANES:WIDE]], axis=0).T
    ssq[0] = jnp.zeros((TOK, LANES), F32)
    ssq[1] = jnp.zeros((TOK, LANES), F32)
    get_wk.wait()
    for get in (get_wv, get_ctx, get_cwk, get_cwv):
        get.start()

    for j in range(6):
        ssq[0] += fold_sq(dot(ybuf[mine], wk[:, tile256(j)]) + vec[BK:BK + 1, tile256(j)])
    k_inv = inv_rms(ssq[0])
    for part in (0, 1):
        abuf[mine, LANES + part:129 + part] = jnp.broadcast_to(k_inv[part * LANES:(part + 1) * LANES], (LANES, LANES)).T[0:1]
    abuf[mine, 130:136] = jnp.zeros((6, LANES), F32)
    start(mine, YP, AX, X2)
    along_z(lambda to: start(mine, to, AX, X2))
    start(mine, CP, AX)

    get_wq.wait()

    for j in range(6):
        lin = dot(ybuf[mine], wq[:, tile256(j)]) + vec[BQ:BQ + 1, tile256(j)]
        raw[:, tile256(j)] = lin
        ssq[1] += fold_sq(lin)
    q_inv = inv_rms(ssq[1])
    packed = abuf[mine, 0:LANES]
    cos_p = jnp.cos(packed)
    sin_p = jnp.sin(packed)
    for part in (0, 1):
        rows = pl.ds(part * LANES, LANES)
        cos_d, sin_d = over_pairs(cos_p, sin_p, part * 64)
        for h in range(HEADS):
            cols = slice(h * LANES, (h + 1) * LANES)
            val = raw[rows, cols] * q_inv[part * LANES:(part + 1) * LANES] * vec[GQ:GQ + 1, cols]
            q_loc[h // 6, rows, (h % 6) * LANES:(h % 6 + 1) * LANES] = (val * cos_d + swap_pairs(val) * sin_d).astype(BF16)
    send_q = pltpu.make_async_remote_copy(q_loc.at[1 - cc], q_got, qo_s.at[0], qo_r.at[0], device_id=dev[CP], device_id_type=MESH)
    send_q.start()

    def event_a(i, hf):
        slot = slot_a(i)
        parts = (X2,) if hf else (X1, AX)
        got(slot, *parts)
        relay(i, lambda to: start(slot, to, *parts))
        start(slot, CP, *parts)
        if not hf or i == 2:
            start(slot, YP, *parts)
        elif i == 1:
            pl.when(ends)(lambda: start(slot, YP, *parts))

    def event_b(i, hf):
        slot = slot_b(i)
        parts = (X2,) if hf else (X1, AX)
        got(slot, *parts)
        start(slot, CP, *parts)
        if hf and not i:
            leave_ends(lambda to: start(slot, to, X2))

    def event_dual(i):
        slot = slot_b(i)
        got(slot, X2)
        relay(i, lambda to: start(slot, to, X2))
        start(slot, CP, X2)

    for h in range(6):
        cols = slice(h * LANES, (h + 1) * LANES)
        q_t[cols, pl.ds(pl.multiple_of(cc * TOK, TOK), TOK)] = q_loc[cc, :, cols].T
    acc[...] = jnp.zeros_like(acc)
    l_s[...] = jnp.zeros_like(l_s)
    m_s[...] = jnp.full_like(m_s, -jnp.inf)
    send_q.wait_recv()
    for h in range(6):
        cols = slice(h * LANES, (h + 1) * LANES)
        q_t[cols, pl.ds(pl.multiple_of((1 - cc) * TOK, TOK), TOK)] = q_got[:, cols].T
    get_wv.wait()

    def cross_k():
        get_ctx.wait()
        get_cwk.wait()
        ssq[...] = jnp.zeros_like(ssq)

        for j in range(6):
            lin = dot(ctx[...], cwk[:, tile256(j)])
            craw[:, tile256(j)] = lin
            sq = fold_sq(lin)
            ssq[0] += sq[:TOK]
            ssq[1] += sq[TOK:]
        inv_0 = inv_rms(ssq[0])
        inv_1 = inv_rms(ssq[1])

        for j in range(6):
            gain = vec[CGK:CGK + 1, tile256(j)]
            ck[0:TOK, tile256(j)] = (craw[0:TOK, tile256(j)] * inv_0 * gain).astype(BF16)
            ck[TOK:TEXT, tile256(j)] = (craw[TOK:TEXT, tile256(j)] * inv_1 * gain).astype(BF16)
        pltpu.make_async_copy(ck, ck_hbm, loc.at[8]).start()

    def cross_v():
        get_cwv.wait()

        for j in range(6):
            cvt[tile256(j), :] = dot(ctx[...], cwv[:, tile256(j)]).astype(BF16).T
        pltpu.make_async_copy(cvt, cvt_hbm, loc.at[9]).start()

    def on(act, *args):
        return lambda: act(*args)

    at_ends = {2: [on(event_a, 1, 0)], 4: [on(event_a, 1, 1)], 6: [on(event_a, 2, 0)], 8: [on(event_a, 2, 1)],
               9: [on(event_b, 1, 1)], 10: [on(event_a, 3, 0)], 12: [on(event_a, 3, 1)], 15: [on(event_dual, 3)]}
    at_mids = {2: [on(event_a, 1, 0), on(event_a, 2, 0)], 4: [on(event_a, 1, 1), on(event_a, 2, 1)],
               8: [on(event_a, 3, 0), on(event_dual, 1)], 10: [on(event_a, 3, 1)], 12: [on(event_dual, 3)]}
    at_all = {3: [on(event_b, 0, 0)], 5: [on(event_b, 0, 1)], 7: [on(event_b, 1, 0)], 11: [on(event_b, 2, 0)],
              13: [on(event_b, 2, 1)], 14: [on(event_b, 3, 0)]}

    def run(acts):
        def go():
            for act in acts:
                act()
        return go

    def body(it, _):
        first = (15 - it) // 14
        last = it // 14
        mid = 1 - first - last
        r = (it + 2) % 4
        k = (it + 2) // 4 - 1
        is_bd = mid * (r % 2) + last
        hf = mid * (r // 2) + (first + last) * (it % 2)
        idx = mid * (k + 1 - r % 2) + last * 3

        for step in range(2, 16):
            @pl.when(it == step)
            def _(step=step):
                for where, table in ((ends, at_ends), (mids, at_mids)):
                    if step in table:
                        pl.when(where)(run(table[step]))
                run(at_all.get(step, ()))()

        pl.when(it == 4)(cross_k)
        pl.when(it == 8)(cross_v)

        pair_slot = (1 - is_bd) * slot_c(idx) + is_bd * slot_d(idx)

        @pl.when(hf == 0)
        def _():
            got(pair_slot, X1, AX)

        @pl.when(hf == 1)
        def _():
            got(pair_slot, X2)

        y_of = (1 - is_bd) * yy + is_bd * (1 - yy)
        base = z_of(idx) * 4 + y_of * 2

        @pl.when(hf == 0)
        def _():
            for s in (0, 1):
                packed = abuf[base + s, 0:LANES]
                cos_s[is_bd * 2 + s] = jnp.cos(packed)
                sin_s[is_bd * 2 + s] = jnp.sin(packed)
        for s in (0, 1):
            rows = slice(s * LANES, (s + 1) * LANES)
            cos_b[rows], sin_b[rows] = over_pairs(cos_s[is_bd * 2 + s], sin_s[is_bd * 2 + s], hf * 64)
            inv_b[rows] = jnp.broadcast_to(abuf[base + s, pl.ds(LANES + hf, 1)], (LANES, LANES)).T
        y_val = ybuf[pl.ds(base, 2), pl.ds(pl.multiple_of(hf * LANES, LANES), LANES)].reshape(TOK, D)

        def k_dot(hp):
            cols = pl.ds(pl.multiple_of(cc * HALF + hp * WIDE, WIDE), WIDE)
            k_f[:, hp * WIDE:(hp + 1) * WIDE] = dot(y_val, wk[:, cols])

        def k_rope(h):
            cols = pl.ds(pl.multiple_of(cc * HALF + h * LANES, LANES), LANES)
            val = (k_f[:, h * LANES:(h + 1) * LANES] + vec[BK:BK + 1, cols]) * inv_b[...] * vec[GK:GK + 1, cols]
            k_b[:, h * LANES:(h + 1) * LANES] = (val * cos_b[...] + swap_pairs(val) * sin_b[...]).astype(BF16)

        def v_dot(hp):
            cols = pl.ds(pl.multiple_of(cc * HALF + hp * WIDE, WIDE), WIDE)
            wide = slice(hp * WIDE, (hp + 1) * WIDE)
            v_b[:, wide] = (dot(y_val, wv[:, wide]) + vec[BV:BV + 1, cols]).astype(BF16)

        def score(h):
            cols = slice(h * LANES, (h + 1) * LANES)
            sc = dot(k_b[:, cols], q_t[cols])
            sc_s[h % 3] = sc
            m_old = m_s[h]
            m_new = jnp.maximum(m_old, jnp.max(sc, axis=0, keepdims=True) * EXP_SCALE)
            m_s[h] = m_new
            return m_new, jnp.exp2(m_old - m_new)

        def weigh(h, m_new, alpha):
            w = jnp.exp2(sc_s[h % 3] * EXP_SCALE - m_new)
            l_s[h] = l_s[h] * alpha + jnp.sum(w.reshape(32, 8, 2 * TOK), axis=0)
            w_s[h % 2] = w.astype(BF16)

        def add_up(h, alpha):
            cols = slice(h * LANES, (h + 1) * LANES)
            acc[h] = acc[h] * alpha + dot_dims(v_b[:, cols], w_s[h % 2], 0, 0)

        for hp in range(3):
            k_dot(hp)
        for hp in range(3):
            v_dot(hp)
        for h in range(6):
            k_rope(h)
        st = {0: score(0), 1: score(1)}
        for h in range(6):
            weigh(h, *st[h])
            if h + 2 < 6:
                st[h + 2] = score(h + 2)
            add_up(h, st[h][1])
        return 0

    lax.fori_loop(0, 16, body, 0)

    for h in range(6):
        cols = slice(h * LANES, (h + 1) * LANES)
        o_h = (acc[h] / jnp.sum(l_s[h], axis=0, keepdims=True)).T.astype(BF16)
        obuf[0, :, cols] = o_h[:TOK]
        obuf[1, :, cols] = o_h[TOK:]
    send_o = pltpu.make_async_remote_copy(obuf.at[1 - cc], o_hbm.at[cc], qo_s.at[1], qo_r.at[1], device_id=dev[CP], device_id_type=MESH)
    got_o = pltpu.make_async_remote_copy(obuf.at[1 - cc], o_hbm.at[1 - cc], qo_s.at[1], qo_r.at[1], device_id=dev[CP], device_id_type=MESH)
    keep_o = pltpu.make_async_copy(obuf.at[cc], o_hbm.at[cc], loc.at[10])
    send_o.start()
    keep_o.start()

    every = (X1, X2, AX)
    sent(mine, YP, *every)
    sent(mine, CP, *every)
    along_z(lambda to: sent(mine, to, *every))
    leave_ends(lambda to: sent(slot_b(0), to, X2))
    for i in range(1, 4):
        relay(i, lambda to, i=i: sent(slot_a(i), to, *every))
        sent(slot_a(i), CP, *every)
        sent(slot_a(i), YP, X1, AX)
    sent(slot_a(2), YP, X2)
    pl.when(ends)(lambda: sent(slot_a(1), YP, X2))

    @pl.when(mids)
    def _():
        for i in (1, 3):
            relay(i, lambda to, i=i: sent(slot_b(i), to, X2))
    for i in range(4):
        sent(slot_b(i), CP, *every)
    send_q.wait_send()
    pltpu.make_async_copy(ck, ck_hbm, loc.at[8]).wait()
    pltpu.make_async_copy(cvt, cvt_hbm, loc.at[9]).wait()
    send_o.wait_send()
    keep_o.wait()
    got_o.wait_recv()


def gather_attention(*args):
    any_spec = pl.BlockSpec(memory_space=pl.ANY)
    vmem_spec = pl.BlockSpec(memory_space=pltpu.VMEM)
    keys = 16 * TOK
    square = pltpu.VMEM((D, D), BF16)
    return pl.pallas_call(
        attn_kernel,
        out_shape=[jax.ShapeDtypeStruct((2, TOK, HALF), BF16), jax.ShapeDtypeStruct((TEXT, D), BF16), jax.ShapeDtypeStruct((D, TEXT), BF16)],
        in_specs=[any_spec] * 8 + [vmem_spec] * 8,
        out_specs=[any_spec] * 3,
        scratch_shapes=[
            pltpu.VMEM((TOK, D), BF16), pltpu.VMEM((HEAD // 2, TOK), F32), pltpu.VMEM((TEXT, D), BF16),
            square, square, pltpu.VMEM((D, HALF), BF16), square, square, pltpu.VMEM((8, D), F32),
            pltpu.VMEM((16, TOK, D), BF16), pltpu.VMEM((16, AUX, LANES), F32), pltpu.VMEM((TOK, D), F32),
            pltpu.VMEM((2, TOK, HALF), BF16), pltpu.VMEM((TOK, HALF), BF16), pltpu.VMEM((HALF, 2 * TOK), BF16),
            pltpu.VMEM((TOK, HALF), BF16), pltpu.VMEM((TOK, HALF), BF16),
            pltpu.VMEM((4, LANES, LANES), F32), pltpu.VMEM((4, LANES, LANES), F32),
            pltpu.VMEM((TOK, LANES), F32), pltpu.VMEM((TOK, LANES), F32), pltpu.VMEM((TOK, LANES), F32),
            pltpu.VMEM((6, HEAD, 2 * TOK), F32), pltpu.VMEM((6, 1, 2 * TOK), F32), pltpu.VMEM((6, 8, 2 * TOK), F32),
            pltpu.VMEM((TOK, HALF), F32), pltpu.VMEM((3, TOK, 2 * TOK), F32), pltpu.VMEM((2, TOK, 2 * TOK), BF16),
            pltpu.VMEM((TEXT, D), F32), pltpu.VMEM((TEXT, D), BF16), pltpu.VMEM((D, TEXT), BF16), pltpu.VMEM((2, TOK, LANES), F32),
            pltpu.VMEM((2, TOK, HALF), BF16),
            pltpu.SemaphoreType.DMA((3, 16)), pltpu.SemaphoreType.DMA((4, 3, 16)), pltpu.SemaphoreType.DMA((11,)),
            pltpu.SemaphoreType.DMA((2,)), pltpu.SemaphoreType.DMA((2,)),
        ],
        cost_estimate=pl.CostEstimate(flops=2 * keys * D * D + 4 * keys * HALF * 2 * TOK, bytes_accessed=10 * D * D, transcendentals=6 * keys * 2 * TOK),
        compiler_params=pltpu.CompilerParams(collective_id=0, has_side_effects=True, vmem_limit_bytes=VMEM_MAX),
        name="gather_attention",
    )(*args)


def tail_kernel(o_hbm, x_hbm, ck_hbm, cvt_hbm, wo_hbm, cwq_hbm, cwo_hbm, w1_hbm, w2_hbm,
                temb_ref, mod_ref, bo_ref, nw_ref, nb_ref, cgq_ref, out_ref,
                o_v, x_v, ck, cvt, wo, cwq, cwo, w1, w2, vec, res, lin, act, u_b, ssq, sc_s, w_s, sems, ring):
    n_ff = FF // FT

    def ff_copies(t, slot):
        cols = pl.ds(pl.multiple_of(t * FT, FT), FT)
        return (pltpu.make_async_copy(w1_hbm.at[:, cols], w1.at[slot], ring.at[0, slot]),
                pltpu.make_async_copy(w2_hbm.at[cols], w2.at[slot], ring.at[1, slot]))

    gets = [pltpu.make_async_copy(src, dst, sems.at[n]) for n, (src, dst) in enumerate(
        ((o_hbm, o_v), (wo_hbm, wo), (x_hbm.at[0], x_v), (cwq_hbm, cwq), (ck_hbm, ck), (cvt_hbm, cvt), (cwo_hbm, cwo)))]
    get_o, get_wo, get_x, get_cwq, get_ck, get_cvt, get_cwo = gets
    for get in (get_o, get_wo, get_x, get_cwq):
        get.start()
    for row in range(6):
        vec[row:row + 1] = ada_row(temb_ref, mod_ref, row)
    BO, NW, NB, CGQ = 6, 7, 8, 9
    for row, ref in ((BO, bo_ref), (NW, nw_ref), (NB, nb_ref), (CGQ, cgq_ref)):
        vec[row:row + 1] = as_row(ref)

    get_o.wait()
    get_wo.wait()
    for get in (get_ck, get_cvt, get_cwo):
        get.start()
    get_x.wait()

    for j in range(6):
        cols = tile256(j)
        prod = dot(o_v[0], wo[0:HALF, cols]) + dot(o_v[1], wo[HALF:D, cols])
        res[:, cols] = x_v[:, cols].astype(F32) + vec[2:3, cols] * (prod + vec[BO:BO + 1, cols])

    for part in range(TOK // 32):
        rows = slice(part * 32, (part + 1) * 32)
        act[rows] = (layer_norm_rows(res[rows]) * vec[NW:NW + 1] + vec[NB:NB + 1]).astype(BF16)
    get_cwq.wait()
    for t in range(RING):
        for get in ff_copies(t, t):
            get.start()
    ssq[...] = jnp.zeros_like(ssq)

    for j in range(6):
        prod = dot(act[...], cwq[:, tile256(j)])
        lin[:, tile256(j)] = prod
        ssq[...] += fold_sq(prod)
    q_inv = inv_rms(ssq[...])
    get_ck.wait()
    get_cvt.wait()

    def score(h):
        cols = slice(h * LANES, (h + 1) * LANES)
        q_h = (lin[:, cols] * q_inv * vec[CGQ:CGQ + 1, cols]).astype(BF16)
        sc = dot_dims(ck[:, cols], q_h, 1, 1)
        sc_s[h % 3] = sc
        return jnp.max(sc, axis=0, keepdims=True) * EXP_SCALE

    def weigh(h, m_row):
        w = jnp.exp2(sc_s[h % 3] * EXP_SCALE - m_row)
        w_s[h % 2] = w.astype(BF16)
        return jnp.sum(w, axis=0, keepdims=True)

    def finish(h, total):
        cols = slice(h * LANES, (h + 1) * LANES)
        act[:, cols] = (dot(cvt[cols, :], w_s[h % 2]) / total).T.astype(BF16)

    m_rows = {0: score(0), 1: score(1)}
    total = None
    for h in range(HEADS):
        total_prev, total = total, weigh(h, m_rows[h])
        if h + 2 < HEADS:
            m_rows[h + 2] = score(h + 2)
        if h:
            finish(h - 1, total_prev)
    finish(HEADS - 1, total)
    get_cwo.wait()

    for j in range(6):
        cols = tile256(j)
        res[:, cols] += dot(act[...], cwo[:, cols])

    for part in range(TOK // 32):
        rows = slice(part * 32, (part + 1) * 32)
        act[rows] = (layer_norm_rows(res[rows]) * (1.0 + vec[4:5]) + vec[3:4]).astype(BF16)
        lin[rows] = jnp.zeros((32, D), F32)

    def ffn(t, _):
        slot = t % RING
        for get in ff_copies(t, slot):
            get.wait()
        for s in range(FT // WIDE):
            cols = slice(s * WIDE, (s + 1) * WIDE)
            u_b[:, cols] = jax.nn.gelu(dot(act[...], w1[slot, :, cols]), approximate=True).astype(BF16)
        for j in range(6):
            cols = slice(j * WIDE, (j + 1) * WIDE)
            lin[:, cols] += dot(u_b[...], w2[slot, :, cols])

        @pl.when(t + RING < n_ff)
        def _():
            for get in ff_copies(t + RING, slot):
                get.start()
        return 0

    lax.fori_loop(0, n_ff, ffn, 0)

    for part in range(TOK // 32):
        rows = slice(part * 32, (part + 1) * 32)
        out_ref[0, rows] = (res[rows] + vec[5:6] * lin[rows]).astype(BF16)


def tail(*args):
    any_spec = pl.BlockSpec(memory_space=pl.ANY)
    vmem_spec = pl.BlockSpec(memory_space=pltpu.VMEM)
    square = pltpu.VMEM((D, D), BF16)
    return pl.pallas_call(
        tail_kernel,
        out_shape=jax.ShapeDtypeStruct((1, TOK, D), BF16),
        in_specs=[any_spec] * 9 + [vmem_spec] * 6,
        out_specs=vmem_spec,
        scratch_shapes=[
            pltpu.VMEM((2, TOK, HALF), BF16), pltpu.VMEM((TOK, D), BF16), pltpu.VMEM((TEXT, D), BF16), pltpu.VMEM((D, TEXT), BF16),
            square, square, square, pltpu.VMEM((RING, D, FT), BF16), pltpu.VMEM((RING, FT, D), BF16), pltpu.VMEM((16, D), F32),
            pltpu.VMEM((TOK, D), F32), pltpu.VMEM((TOK, D), F32), pltpu.VMEM((TOK, D), BF16), pltpu.VMEM((TOK, FT), BF16), pltpu.VMEM((TOK, LANES), F32),
            pltpu.VMEM((3, TEXT, TOK), F32), pltpu.VMEM((2, TEXT, TOK), BF16),
            pltpu.SemaphoreType.DMA((7,)), pltpu.SemaphoreType.DMA((2, RING)),
        ],
        cost_estimate=pl.CostEstimate(flops=4 * TOK * D * FF + 6 * TOK * D * D, bytes_accessed=4 * D * FF + 6 * D * D, transcendentals=TOK * FF),
        compiler_params=pltpu.CompilerParams(vmem_limit_bytes=VMEM_MAX),
        name="tail",
    )(*args)


def solution(mesh):
    tok_spec = P('dp', ('sp', 'uly'), None)
    batch_spec = P('dp', None, None)

    def local_block(tokens, rope_ang, t_emb, block_mod, context, attn_wq, attn_bq, attn_wk, attn_bk, attn_wv, attn_bv, attn_gq, attn_gk, attn_wo, attn_bo, norm3_w, norm3_b, cross_wq, cross_wk, cross_wv, cross_gq, cross_gk, cross_wo, ffn_w1, ffn_w2):
        o_half, cross_k, cross_vt = gather_attention(tokens, rope_ang.T, context, attn_wq, attn_wk, attn_wv, cross_wk, cross_wv, t_emb.reshape(-1), block_mod.reshape(-1), attn_bq, attn_bk, attn_bv, attn_gq, attn_gk, cross_gk)
        return tail(o_half, tokens, cross_k, cross_vt, attn_wo, cross_wq, cross_wo, ffn_w1, ffn_w2, t_emb.reshape(-1), block_mod.reshape(-1), attn_bo, norm3_w, norm3_b, cross_gq)

    in_specs = (tok_spec, P(('sp', 'uly'), None), batch_spec, P(), batch_spec) + (P(),) * 20
    return jax.shard_map(local_block, mesh=mesh, in_specs=in_specs, out_specs=tok_spec, check_vma=False)
```

```python
import math

import jax
import jax.numpy as jnp
from jax import lax
from jax.experimental import pallas as pl
from jax.experimental.pallas import tpu as pltpu
from jax.sharding import PartitionSpec as P

EPS = 1e-6
HEAD = 128
LANES = 128
HEADS = 12
D = 1536
FF = 8960
TOK = 256
WIDE = 256
TEXT = 512
HALF = 768
AUX = 136
FT = 1280
RING = 4
MESH = pl.DeviceIdType.MESH
EXP_SCALE = math.log2(math.e) * HEAD ** -0.5
F32 = jnp.float32
BF16 = jnp.bfloat16
VMEM_MAX = 67043328


def dot(lhs, rhs):
    return jnp.dot(lhs, rhs, preferred_element_type=F32)


def dot_dims(lhs, rhs, l_dim, r_dim):
    return lax.dot_general(lhs, rhs, (((l_dim,), (r_dim,)), ((), ())), preferred_element_type=F32)


def swap_pairs(val):
    lane = lax.broadcasted_iota(jnp.int32, val.shape, 1)
    return jnp.where(lane % 2 == 0, pltpu.roll(val, 127, 1), pltpu.roll(val, 1, 1))


def over_pairs(cos_p, sin_p, base):
    lane = lax.broadcasted_iota(jnp.int32, (LANES, LANES), 1)
    sign = jnp.where(lane % 2 == 0, -1.0, 1.0).astype(F32)
    pair = lane // 2 + base
    return jnp.take_along_axis(cos_p, pair, axis=1), jnp.take_along_axis(sin_p, pair, axis=1) * sign


def layer_norm_rows(x_f32):
    centered = x_f32 - jnp.mean(x_f32, axis=-1, keepdims=True)
    var = jnp.mean(centered * centered, axis=-1, keepdims=True)
    return centered * lax.rsqrt(var + EPS)


def fold_sq(val):
    return val[:, :LANES] * val[:, :LANES] + val[:, LANES:] * val[:, LANES:]


def inv_rms(ssq):
    return lax.rsqrt(jnp.sum(ssq, axis=1, keepdims=True) * (1.0 / D) + EPS)


def tile256(j):
    return slice(j * WIDE, (j + 1) * WIDE)


def ada_row(temb_ref, mod_ref, row):
    cols = slice(row * D, (row + 1) * D)
    return (temb_ref[cols] + mod_ref[cols]).reshape(1, D)


def as_row(ref):
    return ref[...].astype(F32).reshape(1, D)


def attn_kernel(x_hbm, ang_hbm, c_hbm, wq_hbm, wk_hbm, wv_hbm, cwk_hbm, cwv_hbm,
                temb_ref, mod_ref, bq_ref, bk_ref, bv_ref, gq_ref, gk_ref, cgk_ref,
                o_hbm, ck_hbm, cvt_hbm,
                xbuf, ang, ctx, wq, wk, wv, cwk, cwv, vec,
                ybuf, abuf, raw, q_loc, q_got, q_t, k_b, v_b, cos_s, sin_s, cos_b, sin_b, inv_b, acc, m_s, l_s, k_f, sc_s, w_s,
                craw, ck, cvt, ssq, obuf,
                rs, ss, loc, qo_s, qo_r):
    z = lax.axis_index('sp')
    u = lax.axis_index('uly')
    yy = u // 2
    cc = u % 2
    hi = z // 2
    zm = z * (1 - hi) + (3 - z) * hi
    UP, DN, YP, CP = 0, 1, 2, 3
    dev = ({'sp': (z + 1) % 4, 'uly': u}, {'sp': (z + 3) % 4, 'uly': u},
           {'sp': z, 'uly': (1 - yy) * 2 + cc}, {'sp': z, 'uly': yy * 2 + 1 - cc})
    ends = jnp.logical_or(z == 0, z == 3)
    mids = jnp.logical_and(z > 0, z < 3)

    def z_of(i):
        low = i // 2
        m_i = low * i + (1 - low) * (i + zm - 2 * i * zm)
        return m_i * (1 - hi) + (3 - m_i) * hi

    def slot_a(i):
        return z_of(i) * 4 + yy * 2 + cc

    def slot_b(i):
        return z_of(i) * 4 + (1 - yy) * 2 + cc

    def slot_c(i):
        return z_of(i) * 4 + yy * 2 + 1 - cc

    def slot_d(i):
        return z_of(i) * 4 + (1 - yy) * 2 + 1 - cc

    X1, X2, AX = range(3)

    def copy(slot, part, to):
        ref = abuf.at[slot] if part == AX else ybuf.at[slot, pl.ds(part * LANES, LANES)]
        return pltpu.make_async_remote_copy(ref, ref, ss.at[to, part, slot], rs.at[part, slot], device_id=dev[to], device_id_type=MESH)

    def start(slot, to, *parts):
        for part in parts:
            copy(slot, part, to).start()

    def got(slot, *parts):
        for part in parts:
            copy(slot, part, CP).wait_recv()

    def sent(slot, to, *parts):
        for part in parts:
            copy(slot, part, to).wait_send()

    def along_z(act):
        @pl.when(z < 3)
        def _():
            act(UP)

        @pl.when(z > 0)
        def _():
            act(DN)

    def leave_ends(act):
        @pl.when(z == 0)
        def _():
            act(UP)

        @pl.when(z == 3)
        def _():
            act(DN)

    def relay(i, act):
        to_1 = (UP, DN, DN)[i - 1]
        to_2 = (DN, UP, UP)[i - 1]

        @pl.when(z == 1)
        def _():
            act(to_1)

        @pl.when(z == 2)
        def _():
            act(to_2)

    barrier = pltpu.get_barrier_semaphore()
    for to in (YP, CP):
        pl.semaphore_signal(barrier, 1, device_id=dev[to], device_id_type=MESH)
    along_z(lambda to: pl.semaphore_signal(barrier, 1, device_id=dev[to], device_id_type=MESH))

    get_x = pltpu.make_async_copy(x_hbm.at[0], xbuf, loc.at[0])
    get_ang = pltpu.make_async_copy(ang_hbm, ang, loc.at[1])
    get_wk = pltpu.make_async_copy(wk_hbm, wk, loc.at[2])
    get_wq = pltpu.make_async_copy(wq_hbm, wq, loc.at[3])
    get_wv = pltpu.make_async_copy(wv_hbm.at[:, pl.ds(pl.multiple_of(cc * HALF, HALF), HALF)], wv, loc.at[4])
    get_ctx = pltpu.make_async_copy(c_hbm.at[0], ctx, loc.at[5])
    get_cwk = pltpu.make_async_copy(cwk_hbm, cwk, loc.at[6])
    get_cwv = pltpu.make_async_copy(cwv_hbm, cwv, loc.at[7])
    for get in (get_x, get_ang, get_wk):
        get.start()
    BQ, BK, BV, GQ, GK, CGK = range(6)
    for row, ref in enumerate((bq_ref, bk_ref, bv_ref, gq_ref, gk_ref, cgk_ref)):
        vec[row:row + 1] = as_row(ref)
    shift = ada_row(temb_ref, mod_ref, 0)
    scale = 1.0 + ada_row(temb_ref, mod_ref, 1)
    mine = slot_a(0)
    get_x.wait()
    get_wq.start()

    for part in range(TOK // 32):
        rows = slice(part * 32, (part + 1) * 32)
        ybuf[mine, rows] = (layer_norm_rows(xbuf[rows].astype(F32)) * scale + shift).astype(BF16)

    @pl.when(ends)
    def _():
        pl.semaphore_wait(barrier, 3)

    @pl.when(mids)
    def _():
        pl.semaphore_wait(barrier, 4)

    start(mine, YP, X1)
    along_z(lambda to: start(mine, to, X1))
    start(mine, CP, X1, X2)

    get_ang.wait()
    abuf[mine, 0:LANES] = jnp.concatenate([ang[:, 0:LANES], ang[:, LANES:WIDE]], axis=0).T
    ssq[0] = jnp.zeros((TOK, LANES), F32)
    ssq[1] = jnp.zeros((TOK, LANES), F32)
    get_wk.wait()
    for get in (get_wv, get_ctx, get_cwk, get_cwv):
        get.start()

    for j in range(6):
        ssq[0] += fold_sq(dot(ybuf[mine], wk[:, tile256(j)]) + vec[BK:BK + 1, tile256(j)])
    k_inv = inv_rms(ssq[0])
    for part in (0, 1):
        abuf[mine, LANES + part:129 + part] = jnp.broadcast_to(k_inv[part * LANES:(part + 1) * LANES], (LANES, LANES)).T[0:1]
    abuf[mine, 130:136] = jnp.zeros((6, LANES), F32)
    start(mine, YP, AX, X2)
    along_z(lambda to: start(mine, to, AX, X2))
    start(mine, CP, AX)

    get_wq.wait()

    for j in range(6):
        lin = dot(ybuf[mine], wq[:, tile256(j)]) + vec[BQ:BQ + 1, tile256(j)]
        raw[:, tile256(j)] = lin
        ssq[1] += fold_sq(lin)
    q_inv = inv_rms(ssq[1])
    packed = abuf[mine, 0:LANES]
    cos_p = jnp.cos(packed)
    sin_p = jnp.sin(packed)
    for part in (0, 1):
        rows = pl.ds(part * LANES, LANES)
        cos_d, sin_d = over_pairs(cos_p, sin_p, part * 64)
        for h in range(HEADS):
            cols = slice(h * LANES, (h + 1) * LANES)
            val = raw[rows, cols] * q_inv[part * LANES:(part + 1) * LANES] * vec[GQ:GQ + 1, cols]
            q_loc[h // 6, rows, (h % 6) * LANES:(h % 6 + 1) * LANES] = (val * cos_d + swap_pairs(val) * sin_d).astype(BF16)
    send_q = pltpu.make_async_remote_copy(q_loc.at[1 - cc], q_got, qo_s.at[0], qo_r.at[0], device_id=dev[CP], device_id_type=MESH)
    send_q.start()

    def event_a(i, hf):
        slot = slot_a(i)
        parts = (X2,) if hf else (X1, AX)
        got(slot, *parts)
        relay(i, lambda to: start(slot, to, *parts))
        start(slot, CP, *parts)
        if not hf or i == 2:
            start(slot, YP, *parts)
        elif i == 1:
            pl.when(ends)(lambda: start(slot, YP, *parts))

    def event_b(i, hf):
        slot = slot_b(i)
        parts = (X2,) if hf else (X1, AX)
        got(slot, *parts)
        start(slot, CP, *parts)
        if hf and not i:
            leave_ends(lambda to: start(slot, to, X2))

    def event_dual(i):
        slot = slot_b(i)
        got(slot, X2)
        relay(i, lambda to: start(slot, to, X2))
        start(slot, CP, X2)

    for h in range(6):
        cols = slice(h * LANES, (h + 1) * LANES)
        q_t[cols, pl.ds(pl.multiple_of(cc * TOK, TOK), TOK)] = q_loc[cc, :, cols].T
    acc[...] = jnp.zeros_like(acc)
    l_s[...] = jnp.zeros_like(l_s)
    m_s[...] = jnp.full_like(m_s, -jnp.inf)
    send_q.wait_recv()
    for h in range(6):
        cols = slice(h * LANES, (h + 1) * LANES)
        q_t[cols, pl.ds(pl.multiple_of((1 - cc) * TOK, TOK), TOK)] = q_got[:, cols].T
    get_wv.wait()

    def cross_k():
        get_ctx.wait()
        get_cwk.wait()
        ssq[...] = jnp.zeros_like(ssq)

        for j in range(6):
            lin = dot(ctx[...], cwk[:, tile256(j)])
            craw[:, tile256(j)] = lin
            sq = fold_sq(lin)
            ssq[0] += sq[:TOK]
            ssq[1] += sq[TOK:]
        inv_0 = inv_rms(ssq[0])
        inv_1 = inv_rms(ssq[1])

        for j in range(6):
            gain = vec[CGK:CGK + 1, tile256(j)]
            ck[0:TOK, tile256(j)] = (craw[0:TOK, tile256(j)] * inv_0 * gain).astype(BF16)
            ck[TOK:TEXT, tile256(j)] = (craw[TOK:TEXT, tile256(j)] * inv_1 * gain).astype(BF16)
        pltpu.make_async_copy(ck, ck_hbm, loc.at[8]).start()

    def cross_v():
        get_cwv.wait()

        for j in range(6):
            cvt[tile256(j), :] = dot(ctx[...], cwv[:, tile256(j)]).astype(BF16).T
        pltpu.make_async_copy(cvt, cvt_hbm, loc.at[9]).start()

    def on(act, *args):
        return lambda: act(*args)

    at_ends = {2: [on(event_a, 1, 0)], 4: [on(event_a, 1, 1)], 6: [on(event_a, 2, 0)], 8: [on(event_a, 2, 1)],
               9: [on(event_b, 1, 1)], 10: [on(event_a, 3, 0)], 12: [on(event_a, 3, 1)]}
    at_mids = {2: [on(event_a, 1, 0), on(event_a, 2, 0)], 4: [on(event_a, 1, 1), on(event_a, 2, 1)],
               8: [on(event_a, 3, 0), on(event_dual, 1)], 10: [on(event_a, 3, 1)], 12: [on(event_dual, 3)]}
    at_all = {3: [on(event_b, 0, 0)], 5: [on(event_b, 0, 1)], 7: [on(event_b, 1, 0)], 11: [on(event_b, 2, 0)],
              13: [on(event_b, 2, 1)], 14: [on(event_b, 3, 0)]}

    def run(acts):
        def go():
            for act in acts:
                act()
        return go

    def body(it, _):
        first = (15 - it) // 14
        last = it // 14
        mid = 1 - first - last
        r = (it + 2) % 4
        k = (it + 2) // 4 - 1
        is_bd = mid * (r % 2) + last
        hf = mid * (r // 2) + (first + last) * (it % 2)
        idx = mid * (k + 1 - r % 2) + last * 3

        for step in range(2, 16):
            @pl.when(it == step)
            def _(step=step):
                for where, table in ((ends, at_ends), (mids, at_mids)):
                    if step in table:
                        pl.when(where)(run(table[step]))
                run(at_all.get(step, ()))()
                if step == 14:
                    pl.when(ends)(on(event_dual, 3))

        pl.when(it == 4)(cross_k)
        pl.when(it == 8)(cross_v)

        pair_slot = (1 - is_bd) * slot_c(idx) + is_bd * slot_d(idx)

        @pl.when(hf == 0)
        def _():
            got(pair_slot, X1, AX)

        @pl.when(hf == 1)
        def _():
            got(pair_slot, X2)

        y_of = (1 - is_bd) * yy + is_bd * (1 - yy)
        base = z_of(idx) * 4 + y_of * 2

        @pl.when(hf == 0)
        def _():
            for s in (0, 1):
                packed = abuf[base + s, 0:LANES]
                cos_s[is_bd * 2 + s] = jnp.cos(packed)
                sin_s[is_bd * 2 + s] = jnp.sin(packed)
        for s in (0, 1):
            rows = slice(s * LANES, (s + 1) * LANES)
            cos_b[rows], sin_b[rows] = over_pairs(cos_s[is_bd * 2 + s], sin_s[is_bd * 2 + s], hf * 64)
            inv_b[rows] = jnp.broadcast_to(abuf[base + s, pl.ds(LANES + hf, 1)], (LANES, LANES)).T
        y_val = ybuf[pl.ds(base, 2), pl.ds(pl.multiple_of(hf * LANES, LANES), LANES)].reshape(TOK, D)

        def k_dot(hp):
            cols = pl.ds(pl.multiple_of(cc * HALF + hp * WIDE, WIDE), WIDE)
            k_f[:, hp * WIDE:(hp + 1) * WIDE] = dot(y_val, wk[:, cols])

        def k_rope(h):
            cols = pl.ds(pl.multiple_of(cc * HALF + h * LANES, LANES), LANES)
            val = (k_f[:, h * LANES:(h + 1) * LANES] + vec[BK:BK + 1, cols]) * inv_b[...] * vec[GK:GK + 1, cols]
            k_b[:, h * LANES:(h + 1) * LANES] = (val * cos_b[...] + swap_pairs(val) * sin_b[...]).astype(BF16)

        def v_dot(hp):
            cols = pl.ds(pl.multiple_of(cc * HALF + hp * WIDE, WIDE), WIDE)
            wide = slice(hp * WIDE, (hp + 1) * WIDE)
            v_b[:, wide] = (dot(y_val, wv[:, wide]) + vec[BV:BV + 1, cols]).astype(BF16)

        def score(h):
            cols = slice(h * LANES, (h + 1) * LANES)
            sc = dot(k_b[:, cols], q_t[cols])
            sc_s[h % 3] = sc
            m_old = m_s[h]
            m_new = jnp.maximum(m_old, jnp.max(sc, axis=0, keepdims=True) * EXP_SCALE)
            m_s[h] = m_new
            return m_new, jnp.exp2(m_old - m_new)

        def weigh(h, m_new, alpha):
            w = jnp.exp2(sc_s[h % 3] * EXP_SCALE - m_new)
            l_s[h] = l_s[h] * alpha + jnp.sum(w.reshape(32, 8, 2 * TOK), axis=0)
            w_s[h % 2] = w.astype(BF16)

        def add_up(h, alpha):
            cols = slice(h * LANES, (h + 1) * LANES)
            acc[h] = acc[h] * alpha + dot_dims(v_b[:, cols], w_s[h % 2], 0, 0)

        for hp in range(3):
            k_dot(hp)
        for hp in range(3):
            v_dot(hp)
        for h in range(6):
            k_rope(h)
        st = {0: score(0), 1: score(1)}
        for h in range(6):
            weigh(h, *st[h])
            if h + 2 < 6:
                st[h + 2] = score(h + 2)
            add_up(h, st[h][1])
        return 0

    lax.fori_loop(0, 16, body, 0)

    def o_copies(part):
        cols = pl.ds(part * (HALF // 2), HALF // 2)
        away = pltpu.make_async_remote_copy(obuf.at[1 - cc, :, cols], o_hbm.at[cc, :, cols], qo_s.at[1 + part], qo_r.at[1 + part], device_id=dev[CP], device_id_type=MESH)
        return away, pltpu.make_async_copy(obuf.at[cc, :, cols], o_hbm.at[cc, :, cols], loc.at[10 + part])

    for h in range(6):
        cols = slice(h * LANES, (h + 1) * LANES)
        o_h = (acc[h] / jnp.sum(l_s[h], axis=0, keepdims=True)).T.astype(BF16)
        obuf[0, :, cols] = o_h[:TOK]
        obuf[1, :, cols] = o_h[TOK:]
        if h % 3 == 2:
            for put in o_copies(h // 3):
                put.start()

    every = (X1, X2, AX)
    sent(mine, YP, *every)
    sent(mine, CP, *every)
    along_z(lambda to: sent(mine, to, *every))
    leave_ends(lambda to: sent(slot_b(0), to, X2))
    for i in range(1, 4):
        relay(i, lambda to, i=i: sent(slot_a(i), to, *every))
        sent(slot_a(i), CP, *every)
        sent(slot_a(i), YP, X1, AX)
    sent(slot_a(2), YP, X2)
    pl.when(ends)(lambda: sent(slot_a(1), YP, X2))

    @pl.when(mids)
    def _():
        for i in (1, 3):
            relay(i, lambda to, i=i: sent(slot_b(i), to, X2))
    for i in range(4):
        sent(slot_b(i), CP, *every)
    send_q.wait_send()
    pltpu.make_async_copy(ck, ck_hbm, loc.at[8]).wait()
    pltpu.make_async_copy(cvt, cvt_hbm, loc.at[9]).wait()
    for part in (0, 1):
        away, keep = o_copies(part)
        away.wait_send()
        keep.wait()
        away.wait_recv()


def gather_attention(*args):
    any_spec = pl.BlockSpec(memory_space=pl.ANY)
    vmem_spec = pl.BlockSpec(memory_space=pltpu.VMEM)
    keys = 16 * TOK
    square = pltpu.VMEM((D, D), BF16)
    return pl.pallas_call(
        attn_kernel,
        out_shape=[jax.ShapeDtypeStruct((2, TOK, HALF), BF16), jax.ShapeDtypeStruct((TEXT, D), BF16), jax.ShapeDtypeStruct((D, TEXT), BF16)],
        in_specs=[any_spec] * 8 + [vmem_spec] * 8,
        out_specs=[any_spec] * 3,
        scratch_shapes=[
            pltpu.VMEM((TOK, D), BF16), pltpu.VMEM((HEAD // 2, TOK), F32), pltpu.VMEM((TEXT, D), BF16),
            square, square, pltpu.VMEM((D, HALF), BF16), square, square, pltpu.VMEM((8, D), F32),
            pltpu.VMEM((16, TOK, D), BF16), pltpu.VMEM((16, AUX, LANES), F32), pltpu.VMEM((TOK, D), F32),
            pltpu.VMEM((2, TOK, HALF), BF16), pltpu.VMEM((TOK, HALF), BF16), pltpu.VMEM((HALF, 2 * TOK), BF16),
            pltpu.VMEM((TOK, HALF), BF16), pltpu.VMEM((TOK, HALF), BF16),
            pltpu.VMEM((4, LANES, LANES), F32), pltpu.VMEM((4, LANES, LANES), F32),
            pltpu.VMEM((TOK, LANES), F32), pltpu.VMEM((TOK, LANES), F32), pltpu.VMEM((TOK, LANES), F32),
            pltpu.VMEM((6, HEAD, 2 * TOK), F32), pltpu.VMEM((6, 1, 2 * TOK), F32), pltpu.VMEM((6, 8, 2 * TOK), F32),
            pltpu.VMEM((TOK, HALF), F32), pltpu.VMEM((3, TOK, 2 * TOK), F32), pltpu.VMEM((2, TOK, 2 * TOK), BF16),
            pltpu.VMEM((TEXT, D), F32), pltpu.VMEM((TEXT, D), BF16), pltpu.VMEM((D, TEXT), BF16), pltpu.VMEM((2, TOK, LANES), F32),
            pltpu.VMEM((2, TOK, HALF), BF16),
            pltpu.SemaphoreType.DMA((3, 16)), pltpu.SemaphoreType.DMA((4, 3, 16)), pltpu.SemaphoreType.DMA((12,)),
            pltpu.SemaphoreType.DMA((3,)), pltpu.SemaphoreType.DMA((3,)),
        ],
        cost_estimate=pl.CostEstimate(flops=2 * keys * D * D + 4 * keys * HALF * 2 * TOK, bytes_accessed=10 * D * D, transcendentals=6 * keys * 2 * TOK),
        compiler_params=pltpu.CompilerParams(collective_id=0, has_side_effects=True, vmem_limit_bytes=VMEM_MAX),
        name="gather_attention",
    )(*args)


def tail_kernel(o_hbm, x_hbm, ck_hbm, cvt_hbm, wo_hbm, cwq_hbm, cwo_hbm, w1_hbm, w2_hbm,
                temb_ref, mod_ref, bo_ref, nw_ref, nb_ref, cgq_ref, out_ref,
                o_v, x_v, ck, cvt, wo, cwq, cwo, w1, w2, vec, res, lin, act, u_b, ssq, sc_s, w_s, sems, ring):
    n_ff = FF // FT

    def ff_copies(t, slot):
        cols = pl.ds(pl.multiple_of(t * FT, FT), FT)
        return (pltpu.make_async_copy(w1_hbm.at[:, cols], w1.at[slot], ring.at[0, slot]),
                pltpu.make_async_copy(w2_hbm.at[cols], w2.at[slot], ring.at[1, slot]))

    gets = [pltpu.make_async_copy(src, dst, sems.at[n]) for n, (src, dst) in enumerate(
        ((o_hbm, o_v), (x_hbm.at[0], x_v), (cwq_hbm, cwq), (ck_hbm, ck), (cvt_hbm, cvt), (cwo_hbm, cwo)))]
    get_o, get_x, get_cwq, get_ck, get_cvt, get_cwo = gets
    get_wo = []
    for part in range(3):
        cols = slice(part * 2 * WIDE, (part + 1) * 2 * WIDE)
        get_wo.append(pltpu.make_async_copy(wo_hbm.at[:, cols], wo.at[:, cols], sems.at[6 + part]))
    for get in (get_o, get_wo[0], get_x, get_wo[1], get_wo[2]):
        get.start()
    for row in range(6):
        vec[row:row + 1] = ada_row(temb_ref, mod_ref, row)
    BO, NW, NB, CGQ = 6, 7, 8, 9
    for row, ref in ((BO, bo_ref), (NW, nw_ref), (NB, nb_ref), (CGQ, cgq_ref)):
        vec[row:row + 1] = as_row(ref)

    get_o.wait()
    get_x.wait()

    for j in range(6):
        cols = tile256(j)
        if j % 2 == 0:
            get_wo[j // 2].wait()
            for get in ((get_cwq,), (), (get_ck, get_cvt, get_cwo))[j // 2]:
                get.start()
        prod = dot(o_v[0], wo[0:HALF, cols]) + dot(o_v[1], wo[HALF:D, cols])
        res[:, cols] = x_v[:, cols].astype(F32) + vec[2:3, cols] * (prod + vec[BO:BO + 1, cols])

    for part in range(TOK // 32):
        rows = slice(part * 32, (part + 1) * 32)
        act[rows] = (layer_norm_rows(res[rows]) * vec[NW:NW + 1] + vec[NB:NB + 1]).astype(BF16)
    get_cwq.wait()
    for t in range(RING):
        for get in ff_copies(t, t):
            get.start()
    ssq[...] = jnp.zeros_like(ssq)

    for j in range(6):
        prod = dot(act[...], cwq[:, tile256(j)])
        lin[:, tile256(j)] = prod
        ssq[...] += fold_sq(prod)
    q_inv = inv_rms(ssq[...])
    get_ck.wait()
    get_cvt.wait()

    def score(h):
        cols = slice(h * LANES, (h + 1) * LANES)
        q_h = (lin[:, cols] * q_inv * vec[CGQ:CGQ + 1, cols]).astype(BF16)
        sc = dot_dims(ck[:, cols], q_h, 1, 1)
        sc_s[h % 3] = sc
        return jnp.max(sc, axis=0, keepdims=True) * EXP_SCALE

    def weigh(h, m_row):
        w = jnp.exp2(sc_s[h % 3] * EXP_SCALE - m_row)
        w_s[h % 2] = w.astype(BF16)
        return jnp.sum(w, axis=0, keepdims=True)

    def finish(h, total):
        cols = slice(h * LANES, (h + 1) * LANES)
        act[:, cols] = (dot(cvt[cols, :], w_s[h % 2]) / total).T.astype(BF16)

    m_rows = {0: score(0), 1: score(1)}
    total = None
    for h in range(HEADS):
        total_prev, total = total, weigh(h, m_rows[h])
        if h + 2 < HEADS:
            m_rows[h + 2] = score(h + 2)
        if h:
            finish(h - 1, total_prev)
    finish(HEADS - 1, total)
    get_cwo.wait()

    for j in range(6):
        cols = tile256(j)
        res[:, cols] += dot(act[...], cwo[:, cols])

    for part in range(TOK // 32):
        rows = slice(part * 32, (part + 1) * 32)
        act[rows] = (layer_norm_rows(res[rows]) * (1.0 + vec[4:5]) + vec[3:4]).astype(BF16)
        lin[rows] = jnp.zeros((32, D), F32)

    def ffn(t, _):
        slot = t % RING
        for get in ff_copies(t, slot):
            get.wait()
        for s in range(FT // WIDE):
            cols = slice(s * WIDE, (s + 1) * WIDE)
            u_b[:, cols] = jax.nn.gelu(dot(act[...], w1[slot, :, cols]), approximate=True).astype(BF16)
        for j in range(6):
            cols = slice(j * WIDE, (j + 1) * WIDE)
            lin[:, cols] += dot(u_b[...], w2[slot, :, cols])

        @pl.when(t + RING < n_ff)
        def _():
            for get in ff_copies(t + RING, slot):
                get.start()
        return 0

    lax.fori_loop(0, n_ff, ffn, 0)

    for part in range(TOK // 32):
        rows = slice(part * 32, (part + 1) * 32)
        out_ref[0, rows] = (res[rows] + vec[5:6] * lin[rows]).astype(BF16)


def tail(*args):
    any_spec = pl.BlockSpec(memory_space=pl.ANY)
    vmem_spec = pl.BlockSpec(memory_space=pltpu.VMEM)
    square = pltpu.VMEM((D, D), BF16)
    return pl.pallas_call(
        tail_kernel,
        out_shape=jax.ShapeDtypeStruct((1, TOK, D), BF16),
        in_specs=[any_spec] * 9 + [vmem_spec] * 6,
        out_specs=vmem_spec,
        scratch_shapes=[
            pltpu.VMEM((2, TOK, HALF), BF16), pltpu.VMEM((TOK, D), BF16), pltpu.VMEM((TEXT, D), BF16), pltpu.VMEM((D, TEXT), BF16),
            square, square, square, pltpu.VMEM((RING, D, FT), BF16), pltpu.VMEM((RING, FT, D), BF16), pltpu.VMEM((16, D), F32),
            pltpu.VMEM((TOK, D), F32), pltpu.VMEM((TOK, D), F32), pltpu.VMEM((TOK, D), BF16), pltpu.VMEM((TOK, FT), BF16), pltpu.VMEM((TOK, LANES), F32),
            pltpu.VMEM((3, TEXT, TOK), F32), pltpu.VMEM((2, TEXT, TOK), BF16),
            pltpu.SemaphoreType.DMA((9,)), pltpu.SemaphoreType.DMA((2, RING)),
        ],
        cost_estimate=pl.CostEstimate(flops=4 * TOK * D * FF + 6 * TOK * D * D, bytes_accessed=4 * D * FF + 6 * D * D, transcendentals=TOK * FF),
        compiler_params=pltpu.CompilerParams(vmem_limit_bytes=VMEM_MAX),
        name="tail",
    )(*args)


def solution(mesh):
    tok_spec = P('dp', ('sp', 'uly'), None)
    batch_spec = P('dp', None, None)

    def local_block(tokens, rope_ang, t_emb, block_mod, context, attn_wq, attn_bq, attn_wk, attn_bk, attn_wv, attn_bv, attn_gq, attn_gk, attn_wo, attn_bo, norm3_w, norm3_b, cross_wq, cross_wk, cross_wv, cross_gq, cross_gk, cross_wo, ffn_w1, ffn_w2):
        o_half, cross_k, cross_vt = gather_attention(tokens, rope_ang.T, context, attn_wq, attn_wk, attn_wv, cross_wk, cross_wv, t_emb.reshape(-1), block_mod.reshape(-1), attn_bq, attn_bk, attn_bv, attn_gq, attn_gk, cross_gk)
        return tail(o_half, tokens, cross_k, cross_vt, attn_wo, cross_wq, cross_wo, ffn_w1, ffn_w2, t_emb.reshape(-1), block_mod.reshape(-1), attn_bo, norm3_w, norm3_b, cross_gq)

    in_specs = (tok_spec, P(('sp', 'uly'), None), batch_spec, P(), batch_spec) + (P(),) * 20
    return jax.shard_map(local_block, mesh=mesh, in_specs=in_specs, out_specs=tok_spec, check_vma=False)
```
